32 devices in a mesh: gy: 4 (over z), gx: 8 (over y, x, core).
Axes of the slice: x: 2, y: 2, z: 4, core: 2. Of those that a mesh axis runs over, the one named last changes fastest.
Arguments:
- coefficients: float32 [9, 128, 256], P(None, 'gy', 'gx'), may hold values from -2.1 to 2.1
- vectors: float32 [128, 256, 2048], P('gy', 'gx'), may hold values from -6 to 6
Outputs:
- normal: float32 [25, 128, 256], P(None, 'gy', 'gx')
- image: float32 [128, 256, 2048], P('gy', 'gx')
The draws below stay inside these ranges and needn't reach their ends.
All inputs are finite; a program needn't handle non-finite values.
Results may differ from the reference program's by a relative error of at most 0.00002.
Values sent between devices are 32-bit elements; how exact they have to be, the bound alone decides.
A program may use at most 192 MiB of HBM per device.

```python
import math
import jax
import jax.numpy as jnp
from jax import lax

NV = 2048
NX = 128
NY = 256


def block_levels(rng, shape, shards, least, largest):
    def one(axis_at, parts):
        heights = jax.random.uniform(jax.random.fold_in(jax.random.fold_in(rng, 6), axis_at), (parts,), jnp.float32, least / len(shards), largest / len(shards))
        return jnp.repeat(jnp.exp(heights), shape[axis_at] // parts).reshape((-1,) + (1,) * (len(shape) - axis_at - 1))

    loudness = one(*shards[0])
    for cut in shards[1:]:
        loudness = loudness * one(*cut)
    return loudness


def centred(stream_key, shape, spread, limit, cuts=(), held_as=jnp.bfloat16):
    gain = block_levels(stream_key, shape, cuts, -0.22, 0.18) if cuts else 1.0
    drawn = jax.random.normal(stream_key, shape, jnp.float32) * spread * gain
    return jnp.minimum(jnp.maximum(drawn, -limit), limit).astype(held_as)


def setup_inputs(seed: int = 0) -> dict:
    keys = jax.random.split(jax.random.key(seed), 3)
    coefficients = centred(keys[0], (9, NX, NY), 0.35, 2.1, ((1, 4), (2, 8)), jnp.float32)
    vectors = centred(keys[1], (NX, NY, NV), 1.0, 6.0, ((0, 4), (1, 8)), jnp.float32)
    return dict(coefficients=coefficients, vectors=vectors)


def reference(coefficients, vectors):
    row_pos = jnp.arange(NX, dtype=jnp.int32)[:, None]
    col_pos = jnp.arange(NY, dtype=jnp.int32)[None, :]
    pieces = []
    for k in range(9):
        a = k // 3 - 1
        b = k % 3 - 1
        inside = (row_pos + a >= 0) & (row_pos + a < NX) & (col_pos + b >= 0) & (col_pos + b < NY)
        pieces.append(jnp.where(inside, coefficients[k], jnp.zeros_like(coefficients[k])))
    masked = jnp.stack(pieces)
    padded = jnp.pad(masked, ((0, 0), (1, 1), (1, 1)))
    terms = [jnp.zeros((NX, NY), coefficients.dtype) for slot in range(25)]
    for k in range(9):
        a = k // 3 - 1
        b = k % 3 - 1
        for m in range(9):
            e = (m // 3) - (k // 3)
            f = (m % 3) - (k % 3)
            slot_index = (e + 2) * 5 + (f + 2)
            first = padded[k, 1 - a:1 - a + NX, 1 - b:1 - b + NY]
            second = padded[m, 1 - a:1 - a + NX, 1 - b:1 - b + NY]
            terms[slot_index] = terms[slot_index] + first * second
    normal = jnp.stack(terms)
    block = math.gcd(NV, 128)

    def one_block(step, image):
        part = lax.dynamic_slice_in_dim(vectors, step * block, block, 2)
        wide = jnp.pad(part, ((2, 2), (2, 2), (0, 0)))
        total = jnp.zeros((NX, NY, block), vectors.dtype)
        for e in range(-2, 3):
            for f in range(-2, 3):
                slot_index = (e + 2) * 5 + (f + 2)
                total = total + normal[slot_index][:, :, None] * wide[2 + e:2 + e + NX, 2 + f:2 + f + NY, :]
        return lax.dynamic_update_slice_in_dim(image, total, step * block, 2)

    image = lax.fori_loop(0, NV // block, one_block, jnp.zeros_like(vectors))
    return normal, image
```

```python
import functools
import jax
import jax.numpy as jnp
from jax import lax
from jax.experimental import pallas as pl
from jax.experimental.pallas import tpu as pltpu
from jax.sharding import PartitionSpec as P

MESH = pl.DeviceIdType.MESH
CHUNKS = 4
DIRECTIONS = ((1, 0), (-1, 0), (0, 1), (0, -1), (1, 1), (1, -1), (-1, 1), (-1, -1))
EDGE = 8


def slot_of(e, f):
    return (e + 2) * 5 + (f + 2)


def main_kernel(ny, nx, coef_hbm, x_hbm, image, normal, *scratch):
    (
        coef, xbuf, xh, xl, weights, strips, ring, edges, corners, norm, sources,
        high, low, row_band, side_raw, side_band, up, down, side, xrow, xs,
        coef_sem, load_sem, strip_send, strip_recv, send_sem, recv_sem,
    ) = scratch
    rows, cols, lanes = x_hbm.shape
    group = 128 // cols
    lines = rows // group
    tall = weights.shape[1]
    tiles = 2
    width = lanes // CHUNKS
    gy = lax.axis_index("gy")
    gx = lax.axis_index("gx")

    def there(dy, dx):
        y = gy + dy
        x = gx + dx
        return (y >= 0) & (y < ny) & (x >= 0) & (x < nx)

    barrier = pltpu.get_barrier_semaphore()
    count = jnp.int32(0)
    for dy, dx in DIRECTIONS:
        count = count + there(dy, dx).astype(jnp.int32)

        @pl.when(there(dy, dx))
        def _():
            pl.semaphore_signal(barrier, inc=1, device_id={"gy": gy + dy, "gx": gx + dx}, device_id_type=MESH)

    coef_load = pltpu.make_async_copy(coef_hbm, coef, coef_sem)
    coef_load.start()
    loads = []
    for g in range(lines):
        at = pl.ds(g * group, group)
        loads.append(pltpu.make_async_copy(x_hbm.at[at], xbuf.at[at], load_sem.at[g]))

    mine = {1: pl.ds(rows - 2, 2), -1: pl.ds(0, 2)}
    land = {1: pl.ds(0, 2), 0: pl.ds(2, rows), -1: pl.ds(rows + 2, 2)}
    strip_jobs = []
    jobs = [[] for _ in range(CHUNKS)]
    for d, (dy, dx) in enumerate(DIRECTIONS):
        to = {"gy": gy + dy, "gx": gx + dx}
        if dx == 0:
            source = coef_hbm.at[:, pl.ds(rows - 1 if dy > 0 else 0, 1)]
            target = ring.at[0 if dy > 0 else 1]
        elif dy == 0:
            source = strips.at[0 if dx > 0 else 1]
            target = edges.at[0 if dx > 0 else 1]
        else:
            source = strips.at[0 if dx > 0 else 1, pl.ds(lines if dy > 0 else 0, 1)]
            target = corners.at[d - 4]
        strip_jobs.append(
            pltpu.make_async_remote_copy(
                source, target, strip_send.at[d], strip_recv.at[d], device_id=to, device_id_type=MESH
            )
        )
        for n in range(CHUNKS):
            part = pl.ds(n * width, width)
            if dx == 0:
                source = x_hbm.at[mine[dy], :, part]
                target = (up if dy > 0 else down).at[:, :, part]
            else:
                taken = mine[dy] if dy else pl.ds(0, rows)
                source = x_hbm.at[taken, pl.ds(cols - 2 if dx > 0 else 0, 2), part]
                target = side.at[land[dy], pl.ds(0 if dx > 0 else 2, 2), part]
            jobs[n].append(
                pltpu.make_async_remote_copy(
                    source, target, send_sem.at[n, d], recv_sem.at[n, d], device_id=to, device_id_type=MESH
                )
            )

    def start(copies, chosen):
        for d in chosen:

            @pl.when(there(*DIRECTIONS[d]))
            def _():
                copies[d].start()

    dense = (tall, 128)
    line = lax.broadcasted_iota(jnp.int32, dense, 0)
    lane = lax.broadcasted_iota(jnp.int32, dense, 1)
    place = lane // cols
    column = lane % cols
    row_pos = gy * rows + group * line - 2 + place

    coef_load.wait()
    weights[...] = jnp.zeros_like(weights)
    first = [((i - 2) % group, 0 if i >= 2 else 1) for i in range(group)]
    for k in range(9):
        for i, (row, h) in enumerate(first):
            weights[k, pl.ds(h, lines), i * cols : (i + 1) * cols] = coef[k, pl.ds(row, lines, stride=group), :]
    for s in range(2):
        strip = jnp.zeros(dense, jnp.float32)
        for k in range(9):
            moved = pltpu.roll(weights[k], (k - (cols - 1) * (1 - s)) % 128, 1)
            strip = jnp.where(column == k, moved, strip)
        strips[s] = strip

    pl.semaphore_wait(barrier, count)
    start(strip_jobs, range(8))
    for n in range(CHUNKS):
        start(jobs[n], range(8))
    for load in loads:
        load.start()

    for target, (dy, dx) in (
        (up, (1, 0)), (down, (-1, 0)),
    ):

        @pl.when(jnp.logical_not(there(-dy, -dx)))
        def _():
            target[...] = jnp.zeros_like(target)

    for dy, dx in DIRECTIONS[2:]:

        @pl.when(jnp.logical_not(there(-dy, -dx)))
        def _():
            hole = side.at[land[dy], pl.ds(0 if dx > 0 else 2, 2)]
            hole[...] = jnp.zeros(hole.shape, jnp.float32)

    blank = jnp.zeros((2,) + xh.shape[1:], jnp.bfloat16)
    for ref in (xh, xl):
        ref[0:2] = blank
        ref[rows + 2 : rows + 4] = blank

    for g in range(lines):
        loads[g].wait()

        def split(n, carry):
            part = pl.ds(pl.multiple_of(n * width, width), width)
            block = xbuf[g * group : (g + 1) * group, :, part]
            top = block.astype(jnp.bfloat16)
            xh[g * group + 2 : (g + 1) * group + 2, :, part] = top
            xl[g * group + 2 : (g + 1) * group + 2, :, part] = (block - top.astype(jnp.float32)).astype(jnp.bfloat16)
            return carry

        lax.fori_loop(0, CHUNKS, split, 0)

    for d, (dy, dx) in enumerate(DIRECTIONS):

        @pl.when(there(-dy, -dx))
        def _():
            strip_jobs[d].wait_recv()

    ring_place = {0: (0, 1), 1: (lines, 2)}
    for s, (dy, dx) in enumerate(DIRECTIONS[:2]):
        h, i = ring_place[s]
        for k in range(9):
            weights[k, pl.ds(h, 1), i * cols : (i + 1) * cols] = jnp.where(there(-dy, -dx), ring[s, k], 0.0)
    sides = []
    for s in range(2):
        dx = 1 - 2 * s
        strip = jnp.where(there(0, -dx), edges[s], 0.0)
        for t in range(2):
            dy = 1 - 2 * t
            h, i = ring_place[t]
            corner = corners[DIRECTIONS.index((dy, dx)) - 4]
            corner = jnp.where(there(-dy, -dx), jnp.broadcast_to(corner, dense), 0.0)
            strip = jnp.where((line == h) & (place == i), corner, strip)
        sides.append(strip)

    def inside(a, b, col_pos):
        row = row_pos + a
        col = col_pos + b
        return (row >= 0) & (row < ny * rows) & (col >= 0) & (col < nx * cols)

    def down_rows(value, a):
        if a == 0:
            return value
        moved = pltpu.roll(value, (a * cols) % 128, 1)
        crossed = pltpu.roll(moved, a % tall, 0)
        return jnp.where(place == (0 if a > 0 else group - 1), crossed, moved)

    col_pos = gx * cols + column
    kept = []
    for k in range(9):
        a = k // 3 - 1
        b = k % 3 - 1
        own = jnp.where(inside(a, b, col_pos), weights[k], 0.0)
        before = pltpu.roll(sides[0], (-k) % 128, 1)
        before = jnp.where(inside(a, b, gx * cols - 1), before, 0.0)
        after = pltpu.roll(sides[1], (cols - 1 - k) % 128, 1)
        after = jnp.where(inside(a, b, (gx + 1) * cols), after, 0.0)
        right = jnp.where(column == 0, before, pltpu.roll(own, 1, 1))
        left = jnp.where(column == cols - 1, after, pltpu.roll(own, 127, 1))
        kept.append((left, own, right))
    terms = [None] * 25
    for k in range(9):
        a = k // 3 - 1
        b = k % 3 - 1
        moved = [down_rows(kept[m][b + 1], a) for m in range(9)]
        for m in range(9):
            slot = slot_of(m // 3 - k // 3, m % 3 - k % 3)
            product = moved[k] * moved[m]
            terms[slot] = product if terms[slot] is None else terms[slot] + product
    for slot in range(25):
        norm[slot] = terms[slot]

    for rr in range(group):
        for f in range(-2, 3):
            for t in range(tiles):
                total = jnp.zeros(dense, jnp.float32)
                for i in range(group):
                    e = t * group + i - 2 - rr
                    if -2 <= e <= 2:
                        total = jnp.where(place == i, norm[slot_of(-e, -f)], total)
                sources[rr, f + 2, t] = total

    shape = (cols, 128)
    lane_b = lax.broadcasted_iota(jnp.int32, shape, 1)
    offset = lane_b % cols - lax.broadcasted_iota(jnp.int32, shape, 0)

    def band(g, rr, t):
        total = jnp.zeros(shape, jnp.float32)
        for f in range(-2, 3):
            source = sources[rr, f + 2, t, pl.ds(g + t, 1), :]
            total = jnp.where(offset == f, jnp.broadcast_to(source, shape), total)
        return total

    def two(value):
        top = value.astype(jnp.bfloat16).astype(jnp.float32)
        return top, value - top

    def build(g, carry):
        for rr in range(group):
            for t in range(tiles):
                top, rest = two(band(g, rr, t))
                at = (g, pl.ds(rr * cols, cols), pl.ds(t * 128, 128))
                high[at] = top.astype(jnp.bfloat16)
                low[at] = rest.astype(jnp.bfloat16)
        return carry

    lax.fori_loop(0, lines, build, 0)

    depth = 2 * cols
    for s in range(2):
        for n in range(2):
            value = band(0, n, 0) if s == 0 else band(lines - 1, group - 2 + n, 1)
            if s:
                value = pltpu.roll(value, 128 - depth, 1)
            top, rest = two(jnp.where(lane_b < depth, value, 0.0))
            at = pl.ds(n * cols, cols)
            row_band[s, at, 0:128] = (top + pltpu.roll(top, depth, 1)).astype(jnp.bfloat16)
            row_band[s, at, 128:256] = rest.astype(jnp.bfloat16)

    side_raw[...] = jnp.zeros_like(side_raw)
    thin = (lines, 128)
    lane_s = lax.broadcasted_iota(jnp.int32, thin, 1)
    pairs = ((0, 0, -2), (0, 1, -1), (1, 1, -2), (cols - 2, 2, 2), (cols - 1, 2, 1), (cols - 1, 3, 2))
    for rr in range(group):
        h = (rr + 2) // group
        i = (rr + 2) % group
        for c in (0, 1, cols - 2, cols - 1):
            total = jnp.zeros(thin, jnp.float32)
            for own, j, f in pairs:
                if own != c:
                    continue
                for e in range(-2, 3):
                    wanted = (lane_s // 16 == rr + 2 + e) & (lane_s % 4 == j) & (lane_s % 16 < 12)
                    at = i * cols + c
                    value = norm[slot_of(e, f), pl.ds(h, lines), :][:, at : at + 1]
                    total = jnp.where(wanted, jnp.broadcast_to(value, thin), total)
            spot = rr * 2 * EDGE + (c if c < 2 else c - cols + 2 * EDGE)
            side_raw[pl.ds(spot, lines, stride=2 * EDGE * group), :] = total
    top, rest = two(side_raw[...])
    part = lax.broadcasted_iota(jnp.int32, side_raw.shape, 1) % 16
    side_band[...] = jnp.where(part < 8, top, rest).astype(jnp.bfloat16)

    dot = functools.partial(jnp.dot, preferred_element_type=jnp.float32)

    def local(n, carry):
        part = pl.ds(pl.multiple_of(n * width, width), width)
        for g in range(lines):
            span = pl.ds(g * group, 2 * group)
            h = xh[span, :, part].reshape(2 * group * cols, width)
            l = xl[span, :, part].reshape(2 * group * cols, width)
            total = dot(high[g], h) + dot(low[g], h) + dot(high[g], l)
            image[pl.ds(g * group, group), :, part] = total.reshape(group, cols, width)
        return carry

    lax.fori_loop(0, CHUNKS, local, 0)

    def spread(slot, carry):
        for i, (row, h) in enumerate(first):
            value = norm[slot, pl.ds(h, lines), :]
            normal[slot, pl.ds(row, lines, stride=group), :] = value[:, i * cols : (i + 1) * cols]
        return carry

    lax.fori_loop(0, 25, spread, 0)
    xrow[:, 3 * depth : 4 * depth] = jnp.zeros((2, depth, width), jnp.bfloat16)

    for n in range(CHUNKS):
        for d, (dy, dx) in enumerate(DIRECTIONS):

            @pl.when(there(-dy, -dx))
            def _():
                jobs[n][d].wait_recv()

        part = pl.ds(n * width, width)
        for s, halo in enumerate((up, down)):
            top, rest = two(halo[:, :, part].reshape(depth, width))
            xrow[s, 0:depth] = top.astype(jnp.bfloat16)
            xrow[s, depth : 2 * depth] = rest.astype(jnp.bfloat16)
            xrow[s, 2 * depth : 3 * depth] = top.astype(jnp.bfloat16)
            total = dot(row_band[s], xrow[s])
            at = pl.ds(0 if s == 0 else rows - 2, 2)
            image[at, :, part] = image[at, :, part] + total.reshape(2, cols, width)

        def gather(r, carry):
            raw = side[pl.ds(r * 4, 4), :, part]
            near = lax.broadcasted_iota(jnp.int32, raw.shape, 1) < 4
            raw = jnp.where(near, raw, 0.0)
            top, rest = two(raw)
            both = jnp.concatenate([top[:, 0:4], rest[:, 0:4], top], axis=1)
            xs[pl.ds(r * 4, 4)] = both.astype(jnp.bfloat16)
            return carry

        lax.fori_loop(0, (rows + 4) // 4, gather, 0)

        def beside(g, carry):
            s = xs[pl.ds(g * group, 2 * group)].reshape(2 * group * 16, width)
            total = dot(side_band[pl.ds(pl.multiple_of(g * 64, 64), 64), :], s)
            total = total.reshape(group, 2 * EDGE, width)
            at = pl.ds(g * group, group)
            image[at, 0:EDGE, part] = image[at, 0:EDGE, part] + total[:, 0:EDGE]
            image[at, cols - EDGE : cols, part] = image[at, cols - EDGE : cols, part] + total[:, EDGE:]
            return carry

        lax.fori_loop(0, lines, beside, 0, unroll=True)

    for d, (dy, dx) in enumerate(DIRECTIONS):

        @pl.when(there(dy, dx))
        def _():
            strip_jobs[d].wait_send()
            for n in range(CHUNKS):
                jobs[n][d].wait_send()


def write_kernel(image, normal, image_hbm, normal_hbm, sem):
    rows = image.shape[0]
    pieces = 8
    step = rows // pieces
    copies = [pltpu.make_async_copy(normal, normal_hbm, sem.at[pieces])]
    for n in range(pieces):
        at = pl.ds(n * step, step)
        copies.append(pltpu.make_async_copy(image.at[at], image_hbm.at[at], sem.at[n]))
    for copy in copies:
        copy.start()
    for copy in copies:
        copy.wait()


def per_device(coefficients, vectors):
    rows, cols, lanes = vectors.shape
    ny = lax.axis_size("gy")
    nx = lax.axis_size("gx")
    group = 128 // cols
    lines = rows // group
    tall = -(-(lines + 1) // 8) * 8
    width = lanes // CHUNKS
    real = jnp.float32
    half = jnp.bfloat16
    hbm = pl.BlockSpec(memory_space=pltpu.HBM)
    vmem = pl.BlockSpec(memory_space=pltpu.VMEM)
    image, normal = pl.pallas_call(
        functools.partial(main_kernel, ny, nx),
        out_shape=(pltpu.VMEM(vectors.shape, real), pltpu.VMEM((25, rows, cols), real)),
        in_specs=[hbm, hbm],
        out_specs=(vmem, vmem),
        scratch_shapes=[
            pltpu.VMEM((9, rows, cols), real),
            pltpu.VMEM(vectors.shape, real),
            pltpu.VMEM((rows + 4, cols, lanes), half),
            pltpu.VMEM((rows + 4, cols, lanes), half),
            pltpu.VMEM((9, tall, 128), real),
            pltpu.VMEM((2, tall, 128), real),
            pltpu.VMEM((2, 9, 1, cols), real),
            pltpu.VMEM((2, tall, 128), real),
            pltpu.VMEM((4, 1, 128), real),
            pltpu.VMEM((25, tall, 128), real),
            pltpu.VMEM((group, 5, 2, tall, 128), real),
            pltpu.VMEM((lines, group * cols, 256), half),
            pltpu.VMEM((lines, group * cols, 256), half),
            pltpu.VMEM((2, 2 * cols, 256), half),
            pltpu.VMEM((lines * group * 2 * EDGE, 128), real),
            pltpu.VMEM((lines * group * 2 * EDGE, 128), half),
            pltpu.VMEM((2, cols, lanes), real),
            pltpu.VMEM((2, cols, lanes), real),
            pltpu.VMEM((rows + 4, 8, lanes), real),
            pltpu.VMEM((2, 8 * cols, width), half),
            pltpu.VMEM((rows + 4, 16, width), half),
            pltpu.SemaphoreType.DMA(()),
            pltpu.SemaphoreType.DMA((lines,)),
            pltpu.SemaphoreType.DMA((8,)),
            pltpu.SemaphoreType.DMA((8,)),
            pltpu.SemaphoreType.DMA((CHUNKS, 8)),
            pltpu.SemaphoreType.DMA((CHUNKS, 8)),
        ],
        compiler_params=pltpu.CompilerParams(
            collective_id=0, has_side_effects=True, vmem_limit_bytes=44 * 2**20
        ),
    )(*[pltpu.with_memory_space_constraint(a, pltpu.HBM) for a in (coefficients, vectors)])
    image, normal = pl.pallas_call(
        write_kernel,
        out_shape=(
            jax.ShapeDtypeStruct(vectors.shape, real),
            jax.ShapeDtypeStruct((25, rows, cols), real),
        ),
        in_specs=[vmem, vmem],
        out_specs=(hbm, hbm),
        scratch_shapes=[pltpu.SemaphoreType.DMA((9,))],
        compiler_params=pltpu.CompilerParams(vmem_limit_bytes=4 * 2**20),
    )(*[pltpu.with_memory_space_constraint(a, pltpu.VMEM) for a in (image, normal)])
    return (normal, image)


def solution(mesh):
    in_specs = (P(None, "gy", "gx"), P("gy", "gx", None))
    out_specs = (P(None, "gy", "gx"), P("gy", "gx", None))
    return jax.shard_map(
        per_device, mesh=mesh, in_specs=in_specs, out_specs=out_specs, check_vma=False
    )
```

```python
import functools
import jax
import jax.numpy as jnp
from jax import lax
from jax.experimental import pallas as pl
from jax.experimental.pallas import tpu as pltpu
from jax.sharding import PartitionSpec as P

MESH = pl.DeviceIdType.MESH
PARTS = 2
STEP = 512
DIRECTIONS = ((1, 0), (-1, 0), (0, 1), (0, -1), (1, 1), (1, -1), (-1, 1), (-1, -1))
EDGE = 8


def slot_of(e, f):
    return (e + 2) * 5 + (f + 2)


def two(value):
    top = value.astype(jnp.bfloat16).astype(jnp.float32)
    return top, value - top


def dot(a, b):
    return jnp.dot(a, b, preferred_element_type=jnp.float32)


def row_terms(halo, band, xrow):
    depth = halo.shape[0] * halo.shape[1]
    top, rest = two(halo.reshape(depth, halo.shape[2]))
    xrow[0:depth] = top.astype(jnp.bfloat16)
    xrow[depth : 2 * depth] = rest.astype(jnp.bfloat16)
    xrow[2 * depth : 3 * depth] = top.astype(jnp.bfloat16)
    return dot(band[...], xrow[...]).reshape(halo.shape)


def gather_side(side, part, xs):
    def gather(r, carry):
        raw = side[pl.ds(r * 4, 4), :, part]
        near = lax.broadcasted_iota(jnp.int32, raw.shape, 1) < 4
        top, rest = two(jnp.where(near, raw, 0.0))
        both = jnp.concatenate([top[:, 0:4], rest[:, 0:4], top], axis=1)
        xs[pl.ds(r * 4, 4)] = both.astype(jnp.bfloat16)
        return carry

    lax.fori_loop(0, side.shape[0] // 4, gather, 0)


def side_terms(g, group, side_band, xs):
    width = xs.shape[2]
    s = xs[pl.ds(g * group, 2 * group)].reshape(2 * group * 16, width)
    count = group * 2 * EDGE
    total = dot(side_band[g * count : (g + 1) * count, :], s)
    return total.reshape(group, 2 * EDGE, width)


def main_kernel(ny, nx, coef_hbm, x_hbm, *refs):
    (
        image, normal, up_tail, down_tail, side_tail, row_band, side_band,
        coef, xbuf, xh, xl, weights, strips, ring, edges, corners, norm, sources,
        high, low, side_raw, up_head, down_head, side_head, xrow, xs,
        coef_sem, load_sem, strip_send, strip_recv, send_sem, recv_sem,
    ) = refs
    halos = ((up_head, down_head, side_head), (up_tail, down_tail, side_tail))
    rows, cols, lanes = x_hbm.shape
    group = 128 // cols
    lines = rows // group
    tall = weights.shape[1]
    tiles = 2
    width = lanes // PARTS
    gy = lax.axis_index("gy")
    gx = lax.axis_index("gx")

    def there(dy, dx):
        y = gy + dy
        x = gx + dx
        return (y >= 0) & (y < ny) & (x >= 0) & (x < nx)

    barrier = pltpu.get_barrier_semaphore()
    count = jnp.int32(0)
    for dy, dx in DIRECTIONS:
        count = count + there(dy, dx).astype(jnp.int32)

        @pl.when(there(dy, dx))
        def _():
            pl.semaphore_signal(barrier, inc=1, device_id={"gy": gy + dy, "gx": gx + dx}, device_id_type=MESH)

    coef_load = pltpu.make_async_copy(coef_hbm, coef, coef_sem)
    coef_load.start()
    loads = []
    for g in range(lines):
        at = pl.ds(g * group, group)
        loads.append(pltpu.make_async_copy(x_hbm.at[at], xbuf.at[at], load_sem.at[g]))
    for g in (0, lines - 1):
        loads[g].start()

    mine = {1: pl.ds(rows - 2, 2), -1: pl.ds(0, 2)}
    land = {1: pl.ds(0, 2), 0: pl.ds(2, rows), -1: pl.ds(rows + 2, 2)}
    strip_jobs = []
    jobs = [[] for _ in range(PARTS)]
    for d, (dy, dx) in enumerate(DIRECTIONS):
        to = {"gy": gy + dy, "gx": gx + dx}
        if dx == 0:
            source = coef_hbm.at[:, pl.ds(rows - 1 if dy > 0 else 0, 1)]
            target = ring.at[0 if dy > 0 else 1]
        elif dy == 0:
            source = strips.at[0 if dx > 0 else 1]
            target = edges.at[0 if dx > 0 else 1]
        else:
            source = strips.at[0 if dx > 0 else 1, pl.ds(lines if dy > 0 else 0, 1)]
            target = corners.at[d - 4]
        strip_jobs.append(
            pltpu.make_async_remote_copy(
                source, target, strip_send.at[d], strip_recv.at[d], device_id=to, device_id_type=MESH
            )
        )
        for n in range(PARTS):
            part = pl.ds(n * width, width)
            if dx == 0:
                source = xbuf.at[mine[dy], :, part]
                target = halos[n][0 if dy > 0 else 1]
            else:
                taken = mine[dy] if dy else pl.ds(0, rows)
                source = x_hbm.at[taken, pl.ds(cols - 2 if dx > 0 else 0, 2), part]
                target = halos[n][2].at[land[dy], pl.ds(0 if dx > 0 else 2, 2)]
            jobs[n].append(
                pltpu.make_async_remote_copy(
                    source, target, send_sem.at[n, d], recv_sem.at[n, d], device_id=to, device_id_type=MESH
                )
            )

    def start(copies, chosen):
        for d in chosen:

            @pl.when(there(*DIRECTIONS[d]))
            def _():
                copies[d].start()

    dense = (tall, 128)
    line = lax.broadcasted_iota(jnp.int32, dense, 0)
    lane = lax.broadcasted_iota(jnp.int32, dense, 1)
    place = lane // cols
    column = lane % cols
    row_pos = gy * rows + group * line - 2 + place

    coef_load.wait()
    weights[...] = jnp.zeros_like(weights)
    first = [((i - 2) % group, 0 if i >= 2 else 1) for i in range(group)]
    for k in range(9):
        for i, (row, h) in enumerate(first):
            weights[k, pl.ds(h, lines), i * cols : (i + 1) * cols] = coef[k, pl.ds(row, lines, stride=group), :]
    for s in range(2):
        strip = jnp.zeros(dense, jnp.float32)
        for k in range(9):
            moved = pltpu.roll(weights[k], (k - (cols - 1) * (1 - s)) % 128, 1)
            strip = jnp.where(column == k, moved, strip)
        strips[s] = strip

    loads[0].wait()
    loads[lines - 1].wait()
    for load in loads[1 : lines - 1]:
        load.start()
    pl.semaphore_wait(barrier, count)
    start(strip_jobs, range(8))
    for n in range(PARTS):
        start(jobs[n], range(8))

    for up, down, side in halos:
        for target, dy in ((up, 1), (down, -1)):

            @pl.when(jnp.logical_not(there(-dy, 0)))
            def _():
                target[...] = jnp.zeros_like(target)

        for dy, dx in DIRECTIONS[2:]:

            @pl.when(jnp.logical_not(there(-dy, -dx)))
            def _():
                hole = side.at[land[dy], pl.ds(0 if dx > 0 else 2, 2)]
                hole[...] = jnp.zeros(hole.shape, jnp.float32)

    blank = jnp.zeros((2,) + xh.shape[1:], jnp.bfloat16)
    for ref in (xh, xl):
        ref[0:2] = blank
        ref[rows + 2 : rows + 4] = blank

    for g in (0, lines - 1, *range(1, lines - 1)):
        if 0 < g < lines - 1:
            loads[g].wait()

        def split(n, carry):
            part = pl.ds(pl.multiple_of(n * STEP, STEP), STEP)
            top, rest = two(xbuf[g * group : (g + 1) * group, :, part])
            xh[g * group + 2 : (g + 1) * group + 2, :, part] = top.astype(jnp.bfloat16)
            xl[g * group + 2 : (g + 1) * group + 2, :, part] = rest.astype(jnp.bfloat16)
            return carry

        lax.fori_loop(0, lanes // STEP, split, 0)

    for d, (dy, dx) in enumerate(DIRECTIONS):

        @pl.when(there(-dy, -dx))
        def _():
            strip_jobs[d].wait_recv()

    ring_place = {0: (0, 1), 1: (lines, 2)}
    for s, (dy, dx) in enumerate(DIRECTIONS[:2]):
        h, i = ring_place[s]
        for k in range(9):
            weights[k, pl.ds(h, 1), i * cols : (i + 1) * cols] = jnp.where(there(-dy, -dx), ring[s, k], 0.0)
    sides = []
    for s in range(2):
        dx = 1 - 2 * s
        strip = jnp.where(there(0, -dx), edges[s], 0.0)
        for t in range(2):
            dy = 1 - 2 * t
            h, i = ring_place[t]
            corner = corners[DIRECTIONS.index((dy, dx)) - 4]
            corner = jnp.where(there(-dy, -dx), jnp.broadcast_to(corner, dense), 0.0)
            strip = jnp.where((line == h) & (place == i), corner, strip)
        sides.append(strip)

    def inside(a, b, col_pos):
        row = row_pos + a
        col = col_pos + b
        return (row >= 0) & (row < ny * rows) & (col >= 0) & (col < nx * cols)

    def down_rows(value, a):
        if a == 0:
            return value
        moved = pltpu.roll(value, (a * cols) % 128, 1)
        crossed = pltpu.roll(moved, a % tall, 0)
        return jnp.where(place == (0 if a > 0 else group - 1), crossed, moved)

    col_pos = gx * cols + column
    kept = []
    for k in range(9):
        a = k // 3 - 1
        b = k % 3 - 1
        own = jnp.where(inside(a, b, col_pos), weights[k], 0.0)
        before = pltpu.roll(sides[0], (-k) % 128, 1)
        before = jnp.where(inside(a, b, gx * cols - 1), before, 0.0)
        after = pltpu.roll(sides[1], (cols - 1 - k) % 128, 1)
        after = jnp.where(inside(a, b, (gx + 1) * cols), after, 0.0)
        right = jnp.where(column == 0, before, pltpu.roll(own, 1, 1))
        left = jnp.where(column == cols - 1, after, pltpu.roll(own, 127, 1))
        kept.append((left, own, right))
    terms = [None] * 25
    for k in range(9):
        a = k // 3 - 1
        b = k % 3 - 1
        moved = [down_rows(kept[m][b + 1], a) for m in range(9)]
        for m in range(9):
            slot = slot_of(m // 3 - k // 3, m % 3 - k % 3)
            product = moved[k] * moved[m]
            terms[slot] = product if terms[slot] is None else terms[slot] + product
    for slot in range(25):
        norm[slot] = terms[slot]

    for rr in range(group):
        for f in range(-2, 3):
            for t in range(tiles):
                total = jnp.zeros(dense, jnp.float32)
                for i in range(group):
                    e = t * group + i - 2 - rr
                    if -2 <= e <= 2:
                        total = jnp.where(place == i, norm[slot_of(-e, -f)], total)
                sources[rr, f + 2, t] = total

    shape = (cols, 128)
    lane_b = lax.broadcasted_iota(jnp.int32, shape, 1)
    offset = lane_b % cols - lax.broadcasted_iota(jnp.int32, shape, 0)

    def band(g, rr, t):
        total = jnp.zeros(shape, jnp.float32)
        for f in range(-2, 3):
            source = sources[rr, f + 2, t, pl.ds(g + t, 1), :]
            total = jnp.where(offset == f, jnp.broadcast_to(source, shape), total)
        return total

    def build(g, carry):
        for rr in range(group):
            for t in range(tiles):
                top, rest = two(band(g, rr, t))
                at = (g, pl.ds(rr * cols, cols), pl.ds(t * 128, 128))
                high[at] = top.astype(jnp.bfloat16)
                low[at] = rest.astype(jnp.bfloat16)
        return carry

    lax.fori_loop(0, lines, build, 0)

    depth = 2 * cols
    for s in range(2):
        for n in range(2):
            value = band(0, n, 0) if s == 0 else band(lines - 1, group - 2 + n, 1)
            if s:
                value = pltpu.roll(value, 128 - depth, 1)
            top, rest = two(jnp.where(lane_b < depth, value, 0.0))
            at = pl.ds(n * cols, cols)
            row_band[s, at, 0:128] = (top + pltpu.roll(top, depth, 1)).astype(jnp.bfloat16)
            row_band[s, at, 128:256] = rest.astype(jnp.bfloat16)

    side_raw[...] = jnp.zeros_like(side_raw)
    thin = (lines, 128)
    lane_s = lax.broadcasted_iota(jnp.int32, thin, 1)
    pairs = ((0, 0, -2), (0, 1, -1), (1, 1, -2), (cols - 2, 2, 2), (cols - 1, 2, 1), (cols - 1, 3, 2))
    for rr in range(group):
        h = (rr + 2) // group
        i = (rr + 2) % group
        for c in (0, 1, cols - 2, cols - 1):
            total = jnp.zeros(thin, jnp.float32)
            for own, j, f in pairs:
                if own != c:
                    continue
                for e in range(-2, 3):
                    wanted = (lane_s // 16 == rr + 2 + e) & (lane_s % 4 == j) & (lane_s % 16 < 12)
                    at = i * cols + c
                    value = norm[slot_of(e, f), pl.ds(h, lines), :][:, at : at + 1]
                    total = jnp.where(wanted, jnp.broadcast_to(value, thin), total)
            spot = rr * 2 * EDGE + (c if c < 2 else c - cols + 2 * EDGE)
            side_raw[pl.ds(spot, lines, stride=2 * EDGE * group), :] = total
    top, rest = two(side_raw[...])
    part = lax.broadcasted_iota(jnp.int32, side_raw.shape, 1) % 16
    side_band[...] = jnp.where(part < 8, top, rest).astype(jnp.bfloat16)

    def local(n, carry):
        part = pl.ds(pl.multiple_of(n * STEP, STEP), STEP)
        for g in range(lines):
            span = pl.ds(g * group, 2 * group)
            h = xh[span, :, part].reshape(2 * group * cols, STEP)
            l = xl[span, :, part].reshape(2 * group * cols, STEP)
            total = dot(high[g], h) + dot(low[g], h) + dot(high[g], l)
            image[pl.ds(g * group, group), :, part] = total.reshape(group, cols, STEP)
        return carry

    lax.fori_loop(0, lanes // STEP, local, 0)

    def spread(slot, carry):
        for i, (row, h) in enumerate(first):
            value = norm[slot, pl.ds(h, lines), :]
            normal[slot, pl.ds(row, lines, stride=group), :] = value[:, i * cols : (i + 1) * cols]
        return carry

    lax.fori_loop(0, 25, spread, 0)
    xrow[3 * depth : 4 * depth] = jnp.zeros((depth, STEP), jnp.bfloat16)

    for n in range(PARTS):
        for d, (dy, dx) in enumerate(DIRECTIONS):

            @pl.when(there(-dy, -dx))
            def _():
                jobs[n][d].wait_recv()

        if n == PARTS - 1:
            continue

        def beside(m, carry):
            part = pl.ds(pl.multiple_of(m * STEP, STEP), STEP)
            whole = pl.ds(pl.multiple_of(n * width + m * STEP, STEP), STEP)
            for s in range(2):
                at = pl.ds(0 if s == 0 else rows - 2, 2)
                total = row_terms(halos[n][s][:, :, part], row_band.at[s], xrow)
                image[at, :, whole] = image[at, :, whole] + total
            gather_side(halos[n][2], part, xs)
            for g in range(lines):
                total = side_terms(g, group, side_band, xs)
                at = pl.ds(g * group, group)
                image[at, 0:EDGE, whole] = image[at, 0:EDGE, whole] + total[:, 0:EDGE]
                image[at, cols - EDGE : cols, whole] = image[at, cols - EDGE : cols, whole] + total[:, EDGE:]
            return carry

        lax.fori_loop(0, width // STEP, beside, 0)

    for d, (dy, dx) in enumerate(DIRECTIONS):

        @pl.when(there(dy, dx))
        def _():
            strip_jobs[d].wait_send()
            for n in range(PARTS):
                jobs[n][d].wait_send()


def write_kernel(image, normal, up, down, side, row_band, side_band, image_hbm, normal_hbm, *scratch):
    middle, flank, xrow, xs, sem = scratch
    rows, cols, lanes = image.shape
    group = 128 // cols
    lines = rows // group
    width = side.shape[2]
    head = lanes - width
    depth = 2 * cols
    inner = slice(EDGE, cols - EDGE)
    copies = []

    def send(source, *at):
        copies.append(pltpu.make_async_copy(source, image_hbm.at[at], sem.at[len(copies)]))
        copies[-1].start()

    copies.append(pltpu.make_async_copy(normal, normal_hbm, sem.at[0]))
    copies[0].start()
    for g in range(lines):
        at = pl.ds(g * group, group)
        send(image.at[at, :, 0:head], at, slice(None), pl.ds(0, head))
    at = pl.ds(2, rows - 4)
    send(image.at[at, inner, head:lanes], at, inner, pl.ds(head, width))

    xrow[3 * depth : 4 * depth] = jnp.zeros((depth, STEP), jnp.bfloat16)
    for n in range(width // STEP):
        part = pl.ds(n * STEP, STEP)
        whole = pl.ds(head + n * STEP, STEP)
        gather_side(side, part, xs)
        for g in range(lines):
            at = pl.ds(g * group, group)
            total = side_terms(g, group, side_band, xs)
            flank[n, at, 0:EDGE] = image[at, 0:EDGE, whole] + total[:, 0:EDGE]
            flank[n, at, EDGE:] = image[at, cols - EDGE : cols, whole] + total[:, EDGE:]
        for s, halo in enumerate((up, down)):
            at = pl.ds(0 if s == 0 else rows - 2, 2)
            total = row_terms(halo[:, :, part], row_band.at[s], xrow)
            middle[n, s] = image[at, inner, whole] + total[:, inner]
            flank[n, at, 0:EDGE] = flank[n, at, 0:EDGE] + total[:, 0:EDGE]
            flank[n, at, EDGE:] = flank[n, at, EDGE:] + total[:, cols - EDGE :]
            send(middle.at[n, s], at, inner, whole)
        send(flank.at[n, :, 0:EDGE], slice(None), pl.ds(0, EDGE), whole)
        send(flank.at[n, :, EDGE:], slice(None), pl.ds(cols - EDGE, EDGE), whole)
    for copy in copies:
        copy.wait()


def per_device(coefficients, vectors):
    rows, cols, lanes = vectors.shape
    ny = lax.axis_size("gy")
    nx = lax.axis_size("gx")
    group = 128 // cols
    lines = rows // group
    tall = -(-(lines + 1) // 8) * 8
    width = lanes // PARTS
    edge_cells = lines * group * 2 * EDGE
    real = jnp.float32
    half = jnp.bfloat16
    hbm = pl.BlockSpec(memory_space=pltpu.HBM)
    vmem = pl.BlockSpec(memory_space=pltpu.VMEM)
    halo_shapes = (
        pltpu.VMEM((2, cols, width), real),
        pltpu.VMEM((2, cols, width), real),
        pltpu.VMEM((rows + 4, 8, width), real),
    )
    work = (pltpu.VMEM((8 * cols, STEP), half), pltpu.VMEM((rows + 4, 16, STEP), half))
    found = pl.pallas_call(
        functools.partial(main_kernel, ny, nx),
        out_shape=(
            pltpu.VMEM(vectors.shape, real),
            pltpu.VMEM((25, rows, cols), real),
            *halo_shapes,
            pltpu.VMEM((2, 2 * cols, 256), half),
            pltpu.VMEM((edge_cells, 128), half),
        ),
        in_specs=[hbm, hbm],
        out_specs=(vmem,) * 7,
        scratch_shapes=[
            pltpu.VMEM((9, rows, cols), real),
            pltpu.VMEM(vectors.shape, real),
            pltpu.VMEM((rows + 4, cols, lanes), half),
            pltpu.VMEM((rows + 4, cols, lanes), half),
            pltpu.VMEM((9, tall, 128), real),
            pltpu.VMEM((2, tall, 128), real),
            pltpu.VMEM((2, 9, 1, cols), real),
            pltpu.VMEM((2, tall, 128), real),
            pltpu.VMEM((4, 1, 128), real),
            pltpu.VMEM((25, tall, 128), real),
            pltpu.VMEM((group, 5, 2, tall, 128), real),
            pltpu.VMEM((lines, group * cols, 256), half),
            pltpu.VMEM((lines, group * cols, 256), half),
            pltpu.VMEM((edge_cells, 128), real),
            *halo_shapes,
            *work,
            pltpu.SemaphoreType.DMA(()),
            pltpu.SemaphoreType.DMA((lines,)),
            pltpu.SemaphoreType.DMA((8,)),
            pltpu.SemaphoreType.DMA((8,)),
            pltpu.SemaphoreType.DMA((PARTS, 8)),
            pltpu.SemaphoreType.DMA((PARTS, 8)),
        ],
        compiler_params=pltpu.CompilerParams(
            collective_id=0, has_side_effects=True, vmem_limit_bytes=44 * 2**20
        ),
    )(*[pltpu.with_memory_space_constraint(a, pltpu.HBM) for a in (coefficients, vectors)])
    steps = width // STEP
    image, normal = pl.pallas_call(
        write_kernel,
        out_shape=(
            jax.ShapeDtypeStruct(vectors.shape, real),
            jax.ShapeDtypeStruct((25, rows, cols), real),
        ),
        in_specs=[vmem] * 7,
        out_specs=(hbm, hbm),
        scratch_shapes=[
            pltpu.VMEM((steps, 2, 2, cols - 2 * EDGE, STEP), real),
            pltpu.VMEM((steps, rows, 2 * EDGE, STEP), real),
            *work,
            pltpu.SemaphoreType.DMA((2 + lines + 4 * steps,)),
        ],
        compiler_params=pltpu.CompilerParams(vmem_limit_bytes=8 * 2**20),
    )(*[pltpu.with_memory_space_constraint(a, pltpu.VMEM) for a in found])
    return (normal, image)


def solution(mesh):
    in_specs = (P(None, "gy", "gx"), P("gy", "gx", None))
    out_specs = (P(None, "gy", "gx"), P("gy", "gx", None))
    return jax.shard_map(
        per_device, mesh=mesh, in_specs=in_specs, out_specs=out_specs, check_vma=False
    )
```

```python
import functools
import jax
import jax.numpy as jnp
from jax import lax
from jax.experimental import pallas as pl
from jax.experimental.pallas import tpu as pltpu
from jax.sharding import PartitionSpec as P

MESH = pl.DeviceIdType.MESH
PARTS = 2
STEP = 512
ROWWAYS = ((1, 0), (-1, 0))
COLWAYS = ((0, 1), (0, -1))
CORNERS = ((1, 1), (1, -1), (-1, 1), (-1, -1))
EDGE = 8


def slot_of(e, f):
    return (e + 2) * 5 + (f + 2)


def two(value):
    top = value.astype(jnp.bfloat16).astype(jnp.float32)
    return top, value - top


def dot(a, b):
    return jnp.dot(a, b, preferred_element_type=jnp.float32)


def row_terms(halo, band, xrow):
    depth = halo.shape[0] * halo.shape[1]
    top, rest = two(halo.reshape(depth, halo.shape[2]))
    xrow[0:depth] = top.astype(jnp.bfloat16)
    xrow[depth : 2 * depth] = rest.astype(jnp.bfloat16)
    xrow[2 * depth : 3 * depth] = top.astype(jnp.bfloat16)
    return dot(band[...], xrow[...]).reshape(halo.shape)


def gather_side(side, part, xs):
    def gather(r, carry):
        raw = side[pl.ds(r * 4, 4), :, part]
        near = lax.broadcasted_iota(jnp.int32, raw.shape, 1) < 4
        top, rest = two(jnp.where(near, raw, 0.0))
        both = jnp.concatenate([top[:, 0:4], rest[:, 0:4], top], axis=1)
        xs[pl.ds(r * 4, 4)] = both.astype(jnp.bfloat16)
        return carry

    lax.fori_loop(0, side.shape[0] // 4, gather, 0)


def side_terms(g, group, side_band, xs):
    width = xs.shape[2]
    s = xs[pl.ds(g * group, 2 * group)].reshape(2 * group * 16, width)
    count = group * 2 * EDGE
    total = dot(side_band[g * count : (g + 1) * count, :], s)
    return total.reshape(group, 2 * EDGE, width)


def main_kernel(ny, nx, coef_hbm, x_hbm, *refs):
    (
        image, normal, up, down, side, row_band, side_band,
        coef, xbuf, xh, xl, weights, strips, ring, edges, corners, bends, norm,
        sources, high, low, side_raw, xrow, xs,
        coef_sem, load_sem, strip_sems, row_sems, col_sems, relay_sems,
    ) = refs
    rows, cols, lanes = x_hbm.shape
    group = 128 // cols
    lines = rows // group
    tall = weights.shape[1]
    tiles = 2
    width = lanes // PARTS
    gy = lax.axis_index("gy")
    gx = lax.axis_index("gx")

    def there(dy, dx):
        y = gy + dy
        x = gx + dx
        return (y >= 0) & (y < ny) & (x >= 0) & (x < nx)

    barrier = pltpu.get_barrier_semaphore()
    count = jnp.int32(0)
    for dy, dx in ROWWAYS + COLWAYS:
        count = count + there(dy, dx).astype(jnp.int32)

        @pl.when(there(dy, dx))
        def _():
            pl.semaphore_signal(barrier, inc=1, device_id={"gy": gy + dy, "gx": gx + dx}, device_id_type=MESH)

    coef_load = pltpu.make_async_copy(coef_hbm, coef, coef_sem)
    coef_load.start()
    loads = []
    for g in range(lines):
        at = pl.ds(g * group, group)
        loads.append(pltpu.make_async_copy(x_hbm.at[at], xbuf.at[at], load_sem.at[g]))
    for g in (0, lines - 1):
        loads[g].start()

    def job(send, arrive, source, target, dy, dx, sems, *slot):
        copy = pltpu.make_async_remote_copy(
            source, target, sems.at[(0, *slot)], sems.at[(1, *slot)],
            device_id={"gy": gy + dy, "gx": gx + dx}, device_id_type=MESH,
        )
        return send, arrive, copy

    def start(jobs):
        for send, _, copy in jobs:

            @pl.when(send)
            def _():
                copy.start()

    def arrived(jobs):
        for _, arrive, copy in jobs:

            @pl.when(arrive)
            def _():
                copy.wait_recv()

    mine = {1: pl.ds(rows - 2, 2), -1: pl.ds(0, 2)}
    held = {1: pl.ds(rows, 2), -1: pl.ds(2, 2)}
    land = {1: pl.ds(0, 2), -1: pl.ds(rows + 2, 2)}
    spot = {1: pl.ds(0, 2), -1: pl.ds(2, 2)}
    last = {1: pl.ds(cols - 2, 2), -1: pl.ds(0, 2)}
    odd = gx % 2
    near = pl.ds(pl.multiple_of((1 - odd) * (cols - EDGE), EDGE), EDGE)
    far = pl.ds(pl.multiple_of(odd * EDGE, EDGE), cols - EDGE)
    row_strips, col_strips, row_near, row_far, col_ends, col_bulk = [], [], [], [[], []], [], [[], []]
    for n, (dy, dx) in enumerate(ROWWAYS):
        send, arrive = there(dy, dx), there(-dy, -dx)
        halo = up if dy > 0 else down
        row_strips.append(job(
            send, arrive, coef_hbm.at[:, pl.ds(rows - 1 if dy > 0 else 0, 1)], ring.at[n], dy, dx, strip_sems, n
        ))
        row_near.append(job(
            send, arrive, xbuf.at[mine[dy], near], halo.at[:, near], dy, dx, row_sems, n, 0
        ))
        for m in range(PARTS):
            part = pl.ds(m * width, width)
            row_far[m].append(job(
                send, arrive, xbuf.at[mine[dy], far, part], halo.at[:, far, part], dy, dx, row_sems, n, m + 1
            ))
    for n, (dy, dx) in enumerate(COLWAYS):
        send, arrive = there(dy, dx), there(-dy, -dx)
        col_strips.append(job(send, arrive, strips.at[n], edges.at[n], dy, dx, strip_sems, n + 2))
        for m, way in enumerate((1, -1)):
            col_ends.append(job(
                send, arrive, x_hbm.at[mine[way], last[dx]], side.at[held[way], spot[dx]], dy, dx, col_sems, n, m
            ))
        for m in range(PARTS):
            part = pl.ds(m * width, width)
            col_bulk[m].append(job(
                send, arrive, x_hbm.at[pl.ds(2, rows - 4), last[dx], part],
                side.at[pl.ds(4, rows - 4), spot[dx], part], dy, dx, col_sems, n, m + 2
            ))
    turn_x, turn_y, corner_x, corner_y = [], [], [], []
    for n, (dy, dx) in enumerate(CORNERS):
        carrier = odd == (0 if dx > 0 else 1)
        by_x = carrier & there(-dy, 0) & there(0, dx)
        by_y = carrier & there(0, -dx) & there(dy, 0)
        whole = there(-dy, -dx)
        from_x = whole & jnp.logical_not(carrier)
        from_y = whole & carrier
        halo = up if dy > 0 else down
        target = side.at[land[dy], spot[dx]]
        turn_x.append(job(by_x, from_x, halo.at[:, last[dx]], target, 0, dx, relay_sems, n, 0))
        turn_y.append(job(by_y, from_y, side.at[held[dy], spot[dx]], target, dy, 0, relay_sems, n, 1))
        corner_x.append(job(
            by_x, from_x, ring.at[0 if dy > 0 else 1], corners.at[n], 0, dx, relay_sems, n, 2
        ))
        source = edges.at[0 if dx > 0 else 1, pl.ds(lines if dy > 0 else 0, 1)]
        corner_y.append(job(by_y, from_y, source, bends.at[n], dy, 0, relay_sems, n, 3))

    dense = (tall, 128)
    line = lax.broadcasted_iota(jnp.int32, dense, 0)
    lane = lax.broadcasted_iota(jnp.int32, dense, 1)
    place = lane // cols
    column = lane % cols
    row_pos = gy * rows + group * line - 2 + place

    coef_load.wait()
    weights[...] = jnp.zeros_like(weights)
    first = [((i - 2) % group, 0 if i >= 2 else 1) for i in range(group)]
    for k in range(9):
        for i, (row, h) in enumerate(first):
            weights[k, pl.ds(h, lines), i * cols : (i + 1) * cols] = coef[k, pl.ds(row, lines, stride=group), :]
    for s in range(2):
        strip = jnp.zeros(dense, jnp.float32)
        for k in range(9):
            moved = pltpu.roll(weights[k], (k - (cols - 1) * (1 - s)) % 128, 1)
            strip = jnp.where(column == k, moved, strip)
        strips[s] = strip

    loads[0].wait()
    loads[lines - 1].wait()
    for load in loads[1 : lines - 1]:
        load.start()
    pl.semaphore_wait(barrier, count)
    start(row_strips + row_near + col_strips + col_ends)
    for m in range(PARTS):
        start(col_bulk[m])

    for target, dy in ((up, 1), (down, -1)):

        @pl.when(jnp.logical_not(there(-dy, 0)))
        def _():
            target[...] = jnp.zeros_like(target)

    for dx in (1, -1):

        @pl.when(jnp.logical_not(there(0, -dx)))
        def _():
            side[2 : rows + 2, spot[dx]] = jnp.zeros((rows, 2, lanes), jnp.float32)

        for dy in (1, -1):

            @pl.when(jnp.logical_not(there(-dy, -dx)))
            def _():
                side[land[dy], spot[dx]] = jnp.zeros((2, 2, lanes), jnp.float32)

    blank = jnp.zeros((2,) + xh.shape[1:], jnp.bfloat16)
    for ref in (xh, xl):
        ref[0:2] = blank
        ref[rows + 2 : rows + 4] = blank

    for g in (0, lines - 1, *range(1, lines - 1)):
        if 0 < g < lines - 1:
            loads[g].wait()

        def split(n, carry):
            part = pl.ds(pl.multiple_of(n * STEP, STEP), STEP)
            top, rest = two(xbuf[g * group : (g + 1) * group, :, part])
            xh[g * group + 2 : (g + 1) * group + 2, :, part] = top.astype(jnp.bfloat16)
            xl[g * group + 2 : (g + 1) * group + 2, :, part] = rest.astype(jnp.bfloat16)
            return carry

        lax.fori_loop(0, lanes // STEP, split, 0)

    arrived(col_strips + col_ends)
    start(corner_y + turn_y)
    for m in range(PARTS):
        start(row_far[m])
    arrived(row_strips)
    start(corner_x)
    arrived(corner_y + corner_x)

    ring_place = {1: (0, 1), -1: (lines, 2)}
    for n, (dy, dx) in enumerate(ROWWAYS):
        h, i = ring_place[dy]
        for k in range(9):
            weights[k, pl.ds(h, 1), i * cols : (i + 1) * cols] = jnp.where(there(-dy, -dx), ring[n, k], 0.0)
    sides = [jnp.where(there(0, -dx), edges[n], 0.0) for n, (_, dx) in enumerate(COLWAYS)]
    for n, (dy, dx) in enumerate(CORNERS):
        h, i = ring_place[dy]
        here = (line == h) & (place == i)
        at = cols - 1 if dx > 0 else 0
        straight = jnp.zeros(dense, jnp.float32)
        for k in range(9):
            value = jnp.broadcast_to(corners[n, k][:, at : at + 1], dense)
            straight = jnp.where(column == k, value, straight)
        carrier = odd == (0 if dx > 0 else 1)
        value = jnp.where(carrier, jnp.broadcast_to(bends[n], dense), straight)
        value = jnp.where(there(-dy, -dx), value, 0.0)
        s = 0 if dx > 0 else 1
        sides[s] = jnp.where(here, value, sides[s])

    def inside(a, b, col_pos):
        row = row_pos + a
        col = col_pos + b
        return (row >= 0) & (row < ny * rows) & (col >= 0) & (col < nx * cols)

    def down_rows(value, a):
        if a == 0:
            return value
        moved = pltpu.roll(value, (a * cols) % 128, 1)
        crossed = pltpu.roll(moved, a % tall, 0)
        return jnp.where(place == (0 if a > 0 else group - 1), crossed, moved)

    col_pos = gx * cols + column
    kept = []
    for k in range(9):
        a = k // 3 - 1
        b = k % 3 - 1
        own = jnp.where(inside(a, b, col_pos), weights[k], 0.0)
        before = pltpu.roll(sides[0], (-k) % 128, 1)
        before = jnp.where(inside(a, b, gx * cols - 1), before, 0.0)
        after = pltpu.roll(sides[1], (cols - 1 - k) % 128, 1)
        after = jnp.where(inside(a, b, (gx + 1) * cols), after, 0.0)
        right = jnp.where(column == 0, before, pltpu.roll(own, 1, 1))
        left = jnp.where(column == cols - 1, after, pltpu.roll(own, 127, 1))
        kept.append((left, own, right))
    terms = [None] * 25
    for k in range(9):
        a = k // 3 - 1
        b = k % 3 - 1
        moved = [down_rows(kept[m][b + 1], a) for m in range(9)]
        for m in range(9):
            slot = slot_of(m // 3 - k // 3, m % 3 - k % 3)
            product = moved[k] * moved[m]
            terms[slot] = product if terms[slot] is None else terms[slot] + product
    for slot in range(25):
        norm[slot] = terms[slot]

    for rr in range(group):
        for f in range(-2, 3):
            for t in range(tiles):
                total = jnp.zeros(dense, jnp.float32)
                for i in range(group):
                    e = t * group + i - 2 - rr
                    if -2 <= e <= 2:
                        total = jnp.where(place == i, norm[slot_of(-e, -f)], total)
                sources[rr, f + 2, t] = total

    shape = (cols, 128)
    lane_b = lax.broadcasted_iota(jnp.int32, shape, 1)
    offset = lane_b % cols - lax.broadcasted_iota(jnp.int32, shape, 0)

    def band(g, rr, t):
        total = jnp.zeros(shape, jnp.float32)
        for f in range(-2, 3):
            source = sources[rr, f + 2, t, pl.ds(g + t, 1), :]
            total = jnp.where(offset == f, jnp.broadcast_to(source, shape), total)
        return total

    def build(g, carry):
        for rr in range(group):
            for t in range(tiles):
                top, rest = two(band(g, rr, t))
                at = (g, pl.ds(rr * cols, cols), pl.ds(t * 128, 128))
                high[at] = top.astype(jnp.bfloat16)
                low[at] = rest.astype(jnp.bfloat16)
        return carry

    lax.fori_loop(0, lines, build, 0)

    depth = 2 * cols
    for s in range(2):
        for n in range(2):
            value = band(0, n, 0) if s == 0 else band(lines - 1, group - 2 + n, 1)
            if s:
                value = pltpu.roll(value, 128 - depth, 1)
            top, rest = two(jnp.where(lane_b < depth, value, 0.0))
            at = pl.ds(n * cols, cols)
            row_band[s, at, 0:128] = (top + pltpu.roll(top, depth, 1)).astype(jnp.bfloat16)
            row_band[s, at, 128:256] = rest.astype(jnp.bfloat16)

    side_raw[...] = jnp.zeros_like(side_raw)
    thin = (lines, 128)
    lane_s = lax.broadcasted_iota(jnp.int32, thin, 1)
    pairs = ((0, 0, -2), (0, 1, -1), (1, 1, -2), (cols - 2, 2, 2), (cols - 1, 2, 1), (cols - 1, 3, 2))
    for rr in range(group):
        h = (rr + 2) // group
        i = (rr + 2) % group
        for c in (0, 1, cols - 2, cols - 1):
            total = jnp.zeros(thin, jnp.float32)
            for own, j, f in pairs:
                if own != c:
                    continue
                for e in range(-2, 3):
                    wanted = (lane_s // 16 == rr + 2 + e) & (lane_s % 4 == j) & (lane_s % 16 < 12)
                    at = i * cols + c
                    value = norm[slot_of(e, f), pl.ds(h, lines), :][:, at : at + 1]
                    total = jnp.where(wanted, jnp.broadcast_to(value, thin), total)
            spot = rr * 2 * EDGE + (c if c < 2 else c - cols + 2 * EDGE)
            side_raw[pl.ds(spot, lines, stride=2 * EDGE * group), :] = total
    top, rest = two(side_raw[...])
    part = lax.broadcasted_iota(jnp.int32, side_raw.shape, 1) % 16
    side_band[...] = jnp.where(part < 8, top, rest).astype(jnp.bfloat16)

    def local(n, carry):
        part = pl.ds(pl.multiple_of(n * STEP, STEP), STEP)
        for g in range(lines):
            span = pl.ds(g * group, 2 * group)
            h = xh[span, :, part].reshape(2 * group * cols, STEP)
            l = xl[span, :, part].reshape(2 * group * cols, STEP)
            total = dot(high[g], h) + dot(low[g], h) + dot(high[g], l)
            image[pl.ds(g * group, group), :, part] = total.reshape(group, cols, STEP)
        return carry

    lax.fori_loop(0, 1, local, 0)
    arrived(row_near)
    start(turn_x)
    lax.fori_loop(1, lanes // STEP, local, 0)

    def spread(slot, carry):
        for i, (row, h) in enumerate(first):
            value = norm[slot, pl.ds(h, lines), :]
            normal[slot, pl.ds(row, lines, stride=group), :] = value[:, i * cols : (i + 1) * cols]
        return carry

    lax.fori_loop(0, 25, spread, 0)
    xrow[3 * depth : 4 * depth] = jnp.zeros((depth, STEP), jnp.bfloat16)

    arrived(turn_x + turn_y)
    for n in range(PARTS - 1):
        arrived(row_far[n] + col_bulk[n])

        def beside(m, carry):
            part = pl.ds(pl.multiple_of(n * width + m * STEP, STEP), STEP)
            for s, halo in enumerate((up, down)):
                at = pl.ds(0 if s == 0 else rows - 2, 2)
                total = row_terms(halo[:, :, part], row_band.at[s], xrow)
                image[at, :, part] = image[at, :, part] + total
            gather_side(side, part, xs)
            for g in range(lines):
                total = side_terms(g, group, side_band, xs)
                at = pl.ds(g * group, group)
                image[at, 0:EDGE, part] = image[at, 0:EDGE, part] + total[:, 0:EDGE]
                image[at, cols - EDGE : cols, part] = image[at, cols - EDGE : cols, part] + total[:, EDGE:]
            return carry

        lax.fori_loop(0, width // STEP, beside, 0)
    arrived(row_far[PARTS - 1] + col_bulk[PARTS - 1])

    everything = row_strips + col_strips + row_near + col_ends + turn_x + turn_y + corner_x + corner_y
    for m in range(PARTS):
        everything = everything + row_far[m] + col_bulk[m]
    for send, _, copy in everything:

        @pl.when(send)
        def _():
            copy.wait_send()


def write_kernel(image, normal, up, down, side, row_band, side_band, image_hbm, normal_hbm, *scratch):
    middle, flank, xrow, xs, sem = scratch
    rows, cols, lanes = image.shape
    group = 128 // cols
    lines = rows // group
    width = lanes // PARTS
    head = lanes - width
    depth = 2 * cols
    inner = slice(EDGE, cols - EDGE)
    copies = []

    def send(source, *at):
        copies.append(pltpu.make_async_copy(source, image_hbm.at[at], sem.at[len(copies)]))
        copies[-1].start()

    copies.append(pltpu.make_async_copy(normal, normal_hbm, sem.at[0]))
    copies[0].start()
    for g in range(lines):
        at = pl.ds(g * group, group)
        send(image.at[at, :, 0:head], at, slice(None), pl.ds(0, head))
    at = pl.ds(2, rows - 4)
    send(image.at[at, inner, head:lanes], at, inner, pl.ds(head, width))

    xrow[3 * depth : 4 * depth] = jnp.zeros((depth, STEP), jnp.bfloat16)
    for n in range(width // STEP):
        whole = pl.ds(head + n * STEP, STEP)
        gather_side(side, whole, xs)
        for g in range(lines):
            at = pl.ds(g * group, group)
            total = side_terms(g, group, side_band, xs)
            flank[n, at, 0:EDGE] = image[at, 0:EDGE, whole] + total[:, 0:EDGE]
            flank[n, at, EDGE:] = image[at, cols - EDGE : cols, whole] + total[:, EDGE:]
        for s, halo in enumerate((up, down)):
            at = pl.ds(0 if s == 0 else rows - 2, 2)
            total = row_terms(halo[:, :, whole], row_band.at[s], xrow)
            middle[n, s] = image[at, inner, whole] + total[:, inner]
            flank[n, at, 0:EDGE] = flank[n, at, 0:EDGE] + total[:, 0:EDGE]
            flank[n, at, EDGE:] = flank[n, at, EDGE:] + total[:, cols - EDGE :]
            send(middle.at[n, s], at, inner, whole)
        send(flank.at[n, :, 0:EDGE], slice(None), pl.ds(0, EDGE), whole)
        send(flank.at[n, :, EDGE:], slice(None), pl.ds(cols - EDGE, EDGE), whole)
    for copy in copies:
        copy.wait()


def per_device(coefficients, vectors):
    rows, cols, lanes = vectors.shape
    ny = lax.axis_size("gy")
    nx = lax.axis_size("gx")
    group = 128 // cols
    lines = rows // group
    tall = -(-(lines + 1) // 8) * 8
    width = lanes // PARTS
    edge_cells = lines * group * 2 * EDGE
    real = jnp.float32
    half = jnp.bfloat16
    hbm = pl.BlockSpec(memory_space=pltpu.HBM)
    vmem = pl.BlockSpec(memory_space=pltpu.VMEM)
    work = (pltpu.VMEM((8 * cols, STEP), half), pltpu.VMEM((rows + 4, 16, STEP), half))
    found = pl.pallas_call(
        functools.partial(main_kernel, ny, nx),
        out_shape=(
            pltpu.VMEM(vectors.shape, real),
            pltpu.VMEM((25, rows, cols), real),
            pltpu.VMEM((2, cols, lanes), real),
            pltpu.VMEM((2, cols, lanes), real),
            pltpu.VMEM((rows + 4, 8, lanes), real),
            pltpu.VMEM((2, 2 * cols, 256), half),
            pltpu.VMEM((edge_cells, 128), half),
        ),
        in_specs=[hbm, hbm],
        out_specs=(vmem,) * 7,
        scratch_shapes=[
            pltpu.VMEM((9, rows, cols), real),
            pltpu.VMEM(vectors.shape, real),
            pltpu.VMEM((rows + 4, cols, lanes), half),
            pltpu.VMEM((rows + 4, cols, lanes), half),
            pltpu.VMEM((9, tall, 128), real),
            pltpu.VMEM((2, tall, 128), real),
            pltpu.VMEM((2, 9, 1, cols), real),
            pltpu.VMEM((2, tall, 128), real),
            pltpu.VMEM((4, 9, 1, cols), real),
            pltpu.VMEM((4, 1, 128), real),
            pltpu.VMEM((25, tall, 128), real),
            pltpu.VMEM((group, 5, 2, tall, 128), real),
            pltpu.VMEM((lines, group * cols, 256), half),
            pltpu.VMEM((lines, group * cols, 256), half),
            pltpu.VMEM((edge_cells, 128), real),
            *work,
            pltpu.SemaphoreType.DMA(()),
            pltpu.SemaphoreType.DMA((lines,)),
            pltpu.SemaphoreType.DMA((2, 4)),
            pltpu.SemaphoreType.DMA((2, 2, PARTS + 1)),
            pltpu.SemaphoreType.DMA((2, 2, PARTS + 2)),
            pltpu.SemaphoreType.DMA((2, 4, 4)),
        ],
        compiler_params=pltpu.CompilerParams(
            collective_id=0, has_side_effects=True, vmem_limit_bytes=44 * 2**20
        ),
    )(*[pltpu.with_memory_space_constraint(a, pltpu.HBM) for a in (coefficients, vectors)])
    steps = width // STEP
    image, normal = pl.pallas_call(
        write_kernel,
        out_shape=(
            jax.ShapeDtypeStruct(vectors.shape, real),
            jax.ShapeDtypeStruct((25, rows, cols), real),
        ),
        in_specs=[vmem] * 7,
        out_specs=(hbm, hbm),
        scratch_shapes=[
            pltpu.VMEM((steps, 2, 2, cols - 2 * EDGE, STEP), real),
            pltpu.VMEM((steps, rows, 2 * EDGE, STEP), real),
            *work,
            pltpu.SemaphoreType.DMA((2 + lines + 4 * steps,)),
        ],
        compiler_params=pltpu.CompilerParams(vmem_limit_bytes=8 * 2**20),
    )(*[pltpu.with_memory_space_constraint(a, pltpu.VMEM) for a in found])
    return (normal, image)


def solution(mesh):
    in_specs = (P(None, "gy", "gx"), P("gy", "gx", None))
    out_specs = (P(None, "gy", "gx"), P("gy", "gx", None))
    return jax.shard_map(
        per_device, mesh=mesh, in_specs=in_specs, out_specs=out_specs, check_vma=False
    )
```

```python
import functools
import jax
import jax.numpy as jnp
from jax import lax
from jax.experimental import pallas as pl
from jax.experimental.pallas import tpu as pltpu
from jax.sharding import PartitionSpec as P

MESH = pl.DeviceIdType.MESH
PARTS = 2
STEP = 512
EARLY = 256
ROWWAYS = ((1, 0), (-1, 0))
COLWAYS = ((0, 1), (0, -1))
CORNERS = ((1, 1), (1, -1), (-1, 1), (-1, -1))
EDGE = 8


def slot_of(e, f):
    return (e + 2) * 5 + (f + 2)


def two(value):
    top = value.astype(jnp.bfloat16).astype(jnp.float32)
    return top, value - top


def dot(a, b):
    return jnp.dot(a, b, preferred_element_type=jnp.float32)


def row_terms(halo, band, xrow):
    depth = halo.shape[0] * halo.shape[1]
    top, rest = two(halo.reshape(depth, halo.shape[2]))
    xrow[0:depth] = top.astype(jnp.bfloat16)
    xrow[depth : 2 * depth] = rest.astype(jnp.bfloat16)
    xrow[2 * depth : 3 * depth] = top.astype(jnp.bfloat16)
    return dot(band[...], xrow[...]).reshape(halo.shape)


def gather_side(side, part, xs):
    def gather(r, carry):
        raw = side[pl.ds(r * 4, 4), :, part]
        near = lax.broadcasted_iota(jnp.int32, raw.shape, 1) < 4
        top, rest = two(jnp.where(near, raw, 0.0))
        both = jnp.concatenate([top[:, 0:4], rest[:, 0:4], top], axis=1)
        xs[pl.ds(r * 4, 4)] = both.astype(jnp.bfloat16)
        return carry

    lax.fori_loop(0, side.shape[0] // 4, gather, 0)


def side_terms(g, group, side_band, xs):
    width = xs.shape[2]
    s = xs[pl.ds(g * group, 2 * group)].reshape(2 * group * 16, width)
    count = group * 2 * EDGE
    total = dot(side_band[g * count : (g + 1) * count, :], s)
    return total.reshape(group, 2 * EDGE, width)


def main_kernel(ny, nx, coef_hbm, x_hbm, *refs):
    (
        image, normal, up, down, side, row_band, side_band,
        coef, xbuf, xh, xl, weights, strips, ring, edges, corners, bends, norm,
        sources, high, low, side_raw, xrow, xs,
        coef_sem, load_sem, strip_sems, row_sems, col_sems, relay_sems,
    ) = refs
    rows, cols, lanes = x_hbm.shape
    group = 128 // cols
    lines = rows // group
    tall = weights.shape[1]
    tiles = 2
    width = lanes // PARTS
    gy = lax.axis_index("gy")
    gx = lax.axis_index("gx")

    def there(dy, dx):
        y = gy + dy
        x = gx + dx
        return (y >= 0) & (y < ny) & (x >= 0) & (x < nx)

    barrier = pltpu.get_barrier_semaphore()
    count = jnp.int32(0)
    for dy, dx in ROWWAYS + COLWAYS:
        count = count + there(dy, dx).astype(jnp.int32)

        @pl.when(there(dy, dx))
        def _():
            pl.semaphore_signal(barrier, inc=1, device_id={"gy": gy + dy, "gx": gx + dx}, device_id_type=MESH)

    coef_load = pltpu.make_async_copy(coef_hbm, coef, coef_sem)
    coef_load.start()
    loads = []
    for g in range(lines):
        at = pl.ds(g * group, group)
        loads.append(pltpu.make_async_copy(x_hbm.at[at], xbuf.at[at], load_sem.at[g]))
    for g in (0, lines - 1):
        loads[g].start()

    def job(send, arrive, source, target, dy, dx, sems, *slot):
        copy = pltpu.make_async_remote_copy(
            source, target, sems.at[(0, *slot)], sems.at[(1, *slot)],
            device_id={"gy": gy + dy, "gx": gx + dx}, device_id_type=MESH,
        )
        return send, arrive, copy

    def start(jobs):
        for send, _, copy in jobs:

            @pl.when(send)
            def _():
                copy.start()

    def arrived(jobs):
        for _, arrive, copy in jobs:

            @pl.when(arrive)
            def _():
                copy.wait_recv()

    mine = {1: pl.ds(rows - 2, 2), -1: pl.ds(0, 2)}
    held = {1: pl.ds(rows, 2), -1: pl.ds(2, 2)}
    land = {1: pl.ds(0, 2), -1: pl.ds(rows + 2, 2)}
    spot = {1: pl.ds(0, 2), -1: pl.ds(2, 2)}
    last = {1: pl.ds(cols - 2, 2), -1: pl.ds(0, 2)}
    odd = gx % 2
    early = EARLY
    near = pl.ds(pl.multiple_of((1 - odd) * (cols - EDGE), EDGE), EDGE)
    far = pl.ds(pl.multiple_of(odd * EDGE, EDGE), cols - EDGE)
    row_strips, col_strips, row_near, row_far, col_ends, col_bulk = [], [], [], [[], [], []], [], [[], []]
    for n, (dy, dx) in enumerate(ROWWAYS):
        send, arrive = there(dy, dx), there(-dy, -dx)
        halo = up if dy > 0 else down
        row_strips.append(job(
            send, arrive, coef_hbm.at[:, pl.ds(rows - 1 if dy > 0 else 0, 1)], ring.at[n], dy, dx, strip_sems, n
        ))
        row_near.append(job(
            send, arrive, xbuf.at[mine[dy], near], halo.at[:, near], dy, dx, row_sems, n, 0
        ))
        for m, (begin, size) in enumerate(((0, early), (early, width - early), (width, lanes - width))):
            part = pl.ds(begin, size)
            row_far[m].append(job(
                send, arrive, xbuf.at[mine[dy], far, part], halo.at[:, far, part], dy, dx, row_sems, n, m + 1
            ))
    for n, (dy, dx) in enumerate(COLWAYS):
        send, arrive = there(dy, dx), there(-dy, -dx)
        col_strips.append(job(send, arrive, strips.at[n], edges.at[n], dy, dx, strip_sems, n + 2))
        for m, way in enumerate((1, -1)):
            col_ends.append(job(
                send, arrive, x_hbm.at[mine[way], last[dx]], side.at[held[way], spot[dx]], dy, dx, col_sems, n, m
            ))
        for m in range(PARTS):
            part = pl.ds(m * width, width)
            col_bulk[m].append(job(
                send, arrive, x_hbm.at[pl.ds(2, rows - 4), last[dx], part],
                side.at[pl.ds(4, rows - 4), spot[dx], part], dy, dx, col_sems, n, m + 2
            ))
    turn_x, turn_y, corner_x, corner_y = [], [], [], []
    for n, (dy, dx) in enumerate(CORNERS):
        carrier = odd == (0 if dx > 0 else 1)
        by_x = carrier & there(-dy, 0) & there(0, dx)
        by_y = carrier & there(0, -dx) & there(dy, 0)
        whole = there(-dy, -dx)
        from_x = whole & jnp.logical_not(carrier)
        from_y = whole & carrier
        halo = up if dy > 0 else down
        target = side.at[land[dy], spot[dx]]
        turn_x.append(job(by_x, from_x, halo.at[:, last[dx]], target, 0, dx, relay_sems, n, 0))
        turn_y.append(job(by_y, from_y, side.at[held[dy], spot[dx]], target, dy, 0, relay_sems, n, 1))
        corner_x.append(job(
            by_x, from_x, ring.at[0 if dy > 0 else 1], corners.at[n], 0, dx, relay_sems, n, 2
        ))
        source = edges.at[0 if dx > 0 else 1, pl.ds(lines if dy > 0 else 0, 1)]
        corner_y.append(job(by_y, from_y, source, bends.at[n], dy, 0, relay_sems, n, 3))

    dense = (tall, 128)
    line = lax.broadcasted_iota(jnp.int32, dense, 0)
    lane = lax.broadcasted_iota(jnp.int32, dense, 1)
    place = lane // cols
    column = lane % cols
    row_pos = gy * rows + group * line - 2 + place

    coef_load.wait()
    weights[...] = jnp.zeros_like(weights)
    first = [((i - 2) % group, 0 if i >= 2 else 1) for i in range(group)]
    for k in range(9):
        for i, (row, h) in enumerate(first):
            weights[k, pl.ds(h, lines), i * cols : (i + 1) * cols] = coef[k, pl.ds(row, lines, stride=group), :]
    for s in range(2):
        strip = jnp.zeros(dense, jnp.float32)
        for k in range(9):
            moved = pltpu.roll(weights[k], (k - (cols - 1) * (1 - s)) % 128, 1)
            strip = jnp.where(column == k, moved, strip)
        strips[s] = strip

    loads[0].wait()
    loads[lines - 1].wait()
    for load in loads[1 : lines - 1]:
        load.start()
    pl.semaphore_wait(barrier, count)
    start(row_strips + row_near + row_far[0] + col_strips + col_ends)
    for m in range(PARTS):
        start(col_bulk[m])

    for target, dy in ((up, 1), (down, -1)):

        @pl.when(jnp.logical_not(there(-dy, 0)))
        def _():
            target[...] = jnp.zeros_like(target)

    for dx in (1, -1):

        @pl.when(jnp.logical_not(there(0, -dx)))
        def _():
            side[2 : rows + 2, spot[dx]] = jnp.zeros((rows, 2, lanes), jnp.float32)

        for dy in (1, -1):

            @pl.when(jnp.logical_not(there(-dy, -dx)))
            def _():
                side[land[dy], spot[dx]] = jnp.zeros((2, 2, lanes), jnp.float32)

    blank = jnp.zeros((2,) + xh.shape[1:], jnp.bfloat16)
    for ref in (xh, xl):
        ref[0:2] = blank
        ref[rows + 2 : rows + 4] = blank

    for g in (0, lines - 1, *range(1, lines - 1)):
        if 0 < g < lines - 1:
            loads[g].wait()

        def split(n, carry):
            part = pl.ds(pl.multiple_of(n * STEP, STEP), STEP)
            top, rest = two(xbuf[g * group : (g + 1) * group, :, part])
            xh[g * group + 2 : (g + 1) * group + 2, :, part] = top.astype(jnp.bfloat16)
            xl[g * group + 2 : (g + 1) * group + 2, :, part] = rest.astype(jnp.bfloat16)
            return carry

        lax.fori_loop(0, lanes // STEP, split, 0)

    arrived(col_strips + col_ends)
    start(corner_y + turn_y + row_far[1] + row_far[2])
    arrived(row_strips)
    start(corner_x)

    def inside(a, b, col_pos):
        row = row_pos + a
        col = col_pos + b
        return (row >= 0) & (row < ny * rows) & (col >= 0) & (col < nx * cols)

    def down_rows(value, a):
        if a == 0:
            return value
        moved = pltpu.roll(value, (a * cols) % 128, 1)
        crossed = pltpu.roll(moved, a % tall, 0)
        return jnp.where(place == (0 if a > 0 else group - 1), crossed, moved)

    def assemble(sides):
        col_pos = gx * cols + column
        kept = []
        for k in range(9):
            a = k // 3 - 1
            b = k % 3 - 1
            own = jnp.where(inside(a, b, col_pos), weights[k], 0.0)
            before = pltpu.roll(sides[0], (-k) % 128, 1)
            before = jnp.where(inside(a, b, gx * cols - 1), before, 0.0)
            after = pltpu.roll(sides[1], (cols - 1 - k) % 128, 1)
            after = jnp.where(inside(a, b, (gx + 1) * cols), after, 0.0)
            right = jnp.where(column == 0, before, pltpu.roll(own, 1, 1))
            left = jnp.where(column == cols - 1, after, pltpu.roll(own, 127, 1))
            kept.append((left, own, right))
        terms = [None] * 25
        for k in range(9):
            a = k // 3 - 1
            b = k % 3 - 1
            moved = [down_rows(kept[m][b + 1], a) for m in range(9)]
            for m in range(9):
                slot = slot_of(m // 3 - k // 3, m % 3 - k % 3)
                product = moved[k] * moved[m]
                terms[slot] = product if terms[slot] is None else terms[slot] + product
        for slot in range(25):
            norm[slot] = terms[slot]

        for rr in range(group):
            for f in range(-2, 3):
                for t in range(tiles):
                    total = jnp.zeros(dense, jnp.float32)
                    for i in range(group):
                        e = t * group + i - 2 - rr
                        if -2 <= e <= 2:
                            total = jnp.where(place == i, norm[slot_of(-e, -f)], total)
                    sources[rr, f + 2, t] = total

    shape = (cols, 128)
    lane_b = lax.broadcasted_iota(jnp.int32, shape, 1)
    offset = lane_b % cols - lax.broadcasted_iota(jnp.int32, shape, 0)

    def band(g, rr, t):
        total = jnp.zeros(shape, jnp.float32)
        for f in range(-2, 3):
            source = sources[rr, f + 2, t, pl.ds(g + t, 1), :]
            total = jnp.where(offset == f, jnp.broadcast_to(source, shape), total)
        return total

    def build(g, carry):
        for rr in range(group):
            for t in range(tiles):
                top, rest = two(band(g, rr, t))
                at = (g, pl.ds(rr * cols, cols), pl.ds(t * 128, 128))
                high[at] = top.astype(jnp.bfloat16)
                low[at] = rest.astype(jnp.bfloat16)
        return carry


    def local(groups):
        def body(n, carry):
            part = pl.ds(pl.multiple_of(n * STEP, STEP), STEP)
            for g in groups:
                span = pl.ds(g * group, 2 * group)
                h = xh[span, :, part].reshape(2 * group * cols, STEP)
                l = xl[span, :, part].reshape(2 * group * cols, STEP)
                total = dot(high[g], h) + dot(low[g], h) + dot(high[g], l)
                image[pl.ds(g * group, group), :, part] = total.reshape(group, cols, STEP)
            return carry

        return body

    sides = [jnp.where(there(0, -dx), edges[n], 0.0) for n, (_, dx) in enumerate(COLWAYS)]
    assemble(sides)
    lax.fori_loop(1, lines - 1, build, 0)
    inner = range(1, lines - 1)
    lax.fori_loop(0, 2, local(inner), 0)
    arrived(row_near)
    start(turn_x)
    lax.fori_loop(2, lanes // STEP, local(inner), 0)
    arrived(corner_y + corner_x)


    ring_place = {1: (0, 1), -1: (lines, 2)}
    for n, (dy, dx) in enumerate(ROWWAYS):
        h, i = ring_place[dy]
        for k in range(9):
            weights[k, pl.ds(h, 1), i * cols : (i + 1) * cols] = jnp.where(there(-dy, -dx), ring[n, k], 0.0)
    for n, (dy, dx) in enumerate(CORNERS):
        h, i = ring_place[dy]
        here = (line == h) & (place == i)
        at = cols - 1 if dx > 0 else 0
        straight = jnp.zeros(dense, jnp.float32)
        for k in range(9):
            value = jnp.broadcast_to(corners[n, k][:, at : at + 1], dense)
            straight = jnp.where(column == k, value, straight)
        carrier = odd == (0 if dx > 0 else 1)
        value = jnp.where(carrier, jnp.broadcast_to(bends[n], dense), straight)
        value = jnp.where(there(-dy, -dx), value, 0.0)
        s = 0 if dx > 0 else 1
        sides[s] = jnp.where(here, value, sides[s])

    assemble(sides)
    for g in (0, lines - 1):
        build(g, 0)
    lax.fori_loop(0, lanes // STEP, local((0, lines - 1)), 0)

    depth = 2 * cols
    for s in range(2):
        for n in range(2):
            value = band(0, n, 0) if s == 0 else band(lines - 1, group - 2 + n, 1)
            if s:
                value = pltpu.roll(value, 128 - depth, 1)
            top, rest = two(jnp.where(lane_b < depth, value, 0.0))
            at = pl.ds(n * cols, cols)
            row_band[s, at, 0:128] = (top + pltpu.roll(top, depth, 1)).astype(jnp.bfloat16)
            row_band[s, at, 128:256] = rest.astype(jnp.bfloat16)

    side_raw[...] = jnp.zeros_like(side_raw)
    thin = (lines, 128)
    lane_s = lax.broadcasted_iota(jnp.int32, thin, 1)
    pairs = ((0, 0, -2), (0, 1, -1), (1, 1, -2), (cols - 2, 2, 2), (cols - 1, 2, 1), (cols - 1, 3, 2))
    for rr in range(group):
        h = (rr + 2) // group
        i = (rr + 2) % group
        for c in (0, 1, cols - 2, cols - 1):
            total = jnp.zeros(thin, jnp.float32)
            for own, j, f in pairs:
                if own != c:
                    continue
                for e in range(-2, 3):
                    wanted = (lane_s // 16 == rr + 2 + e) & (lane_s % 4 == j) & (lane_s % 16 < 12)
                    at = i * cols + c
                    value = norm[slot_of(e, f), pl.ds(h, lines), :][:, at : at + 1]
                    total = jnp.where(wanted, jnp.broadcast_to(value, thin), total)
            spot = rr * 2 * EDGE + (c if c < 2 else c - cols + 2 * EDGE)
            side_raw[pl.ds(spot, lines, stride=2 * EDGE * group), :] = total
    top, rest = two(side_raw[...])
    part = lax.broadcasted_iota(jnp.int32, side_raw.shape, 1) % 16
    side_band[...] = jnp.where(part < 8, top, rest).astype(jnp.bfloat16)

    def spread(slot, carry):
        for i, (row, h) in enumerate(first):
            value = norm[slot, pl.ds(h, lines), :]
            normal[slot, pl.ds(row, lines, stride=group), :] = value[:, i * cols : (i + 1) * cols]
        return carry

    lax.fori_loop(0, 25, spread, 0, unroll=5)
    xrow[3 * depth : 4 * depth] = jnp.zeros((depth, STEP), jnp.bfloat16)

    arrived(turn_x + turn_y)
    for n in range(PARTS - 1):
        arrived(row_far[0] + row_far[1] + col_bulk[n])

        def beside(m, carry):
            part = pl.ds(pl.multiple_of(n * width + m * STEP, STEP), STEP)
            for s, halo in enumerate((up, down)):
                at = pl.ds(0 if s == 0 else rows - 2, 2)
                total = row_terms(halo[:, :, part], row_band.at[s], xrow)
                image[at, :, part] = image[at, :, part] + total
            gather_side(side, part, xs)
            for g in range(lines):
                total = side_terms(g, group, side_band, xs)
                at = pl.ds(g * group, group)
                image[at, 0:EDGE, part] = image[at, 0:EDGE, part] + total[:, 0:EDGE]
                image[at, cols - EDGE : cols, part] = image[at, cols - EDGE : cols, part] + total[:, EDGE:]
            return carry

        lax.fori_loop(0, width // STEP, beside, 0)
    arrived(row_far[2] + col_bulk[PARTS - 1])

    everything = row_strips + col_strips + row_near + col_ends + turn_x + turn_y + corner_x + corner_y
    for more in row_far + col_bulk:
        everything = everything + more
    for send, _, copy in everything:

        @pl.when(send)
        def _():
            copy.wait_send()


def write_kernel(image, normal, up, down, side, row_band, side_band, image_hbm, normal_hbm, *scratch):
    middle, flank, xrow, xs, sem = scratch
    rows, cols, lanes = image.shape
    group = 128 // cols
    lines = rows // group
    width = lanes // PARTS
    head = lanes - width
    depth = 2 * cols
    inner = slice(EDGE, cols - EDGE)
    copies = []

    def send(source, *at):
        copies.append(pltpu.make_async_copy(source, image_hbm.at[at], sem.at[len(copies)]))
        copies[-1].start()

    copies.append(pltpu.make_async_copy(normal, normal_hbm, sem.at[0]))
    copies[0].start()
    for g in range(lines):
        at = pl.ds(g * group, group)
        send(image.at[at, :, 0:head], at, slice(None), pl.ds(0, head))
    at = pl.ds(2, rows - 4)
    send(image.at[at, inner, head:lanes], at, inner, pl.ds(head, width))

    xrow[3 * depth : 4 * depth] = jnp.zeros((depth, STEP), jnp.bfloat16)
    for n in range(width // STEP):
        whole = pl.ds(head + n * STEP, STEP)
        gather_side(side, whole, xs)
        for g in range(lines):
            at = pl.ds(g * group, group)
            total = side_terms(g, group, side_band, xs)
            flank[n, at, 0:EDGE] = image[at, 0:EDGE, whole] + total[:, 0:EDGE]
            flank[n, at, EDGE:] = image[at, cols - EDGE : cols, whole] + total[:, EDGE:]
        for s, halo in enumerate((up, down)):
            at = pl.ds(0 if s == 0 else rows - 2, 2)
            total = row_terms(halo[:, :, whole], row_band.at[s], xrow)
            middle[n, s] = image[at, inner, whole] + total[:, inner]
            flank[n, at, 0:EDGE] = flank[n, at, 0:EDGE] + total[:, 0:EDGE]
            flank[n, at, EDGE:] = flank[n, at, EDGE:] + total[:, cols - EDGE :]
            send(middle.at[n, s], at, inner, whole)
        send(flank.at[n, :, 0:EDGE], slice(None), pl.ds(0, EDGE), whole)
        send(flank.at[n, :, EDGE:], slice(None), pl.ds(cols - EDGE, EDGE), whole)
    for copy in copies:
        copy.wait()


def per_device(coefficients, vectors):
    rows, cols, lanes = vectors.shape
    ny = lax.axis_size("gy")
    nx = lax.axis_size("gx")
    group = 128 // cols
    lines = rows // group
    tall = -(-(lines + 1) // 8) * 8
    width = lanes // PARTS
    edge_cells = lines * group * 2 * EDGE
    real = jnp.float32
    half = jnp.bfloat16
    hbm = pl.BlockSpec(memory_space=pltpu.HBM)
    vmem = pl.BlockSpec(memory_space=pltpu.VMEM)
    work = (pltpu.VMEM((8 * cols, STEP), half), pltpu.VMEM((rows + 4, 16, STEP), half))
    found = pl.pallas_call(
        functools.partial(main_kernel, ny, nx),
        out_shape=(
            pltpu.VMEM(vectors.shape, real),
            pltpu.VMEM((25, rows, cols), real),
            pltpu.VMEM((2, cols, lanes), real),
            pltpu.VMEM((2, cols, lanes), real),
            pltpu.VMEM((rows + 4, 8, lanes), real),
            pltpu.VMEM((2, 2 * cols, 256), half),
            pltpu.VMEM((edge_cells, 128), half),
        ),
        in_specs=[hbm, hbm],
        out_specs=(vmem,) * 7,
        scratch_shapes=[
            pltpu.VMEM((9, rows, cols), real),
            pltpu.VMEM(vectors.shape, real),
            pltpu.VMEM((rows + 4, cols, lanes), half),
            pltpu.VMEM((rows + 4, cols, lanes), half),
            pltpu.VMEM((9, tall, 128), real),
            pltpu.VMEM((2, tall, 128), real),
            pltpu.VMEM((2, 9, 1, cols), real),
            pltpu.VMEM((2, tall, 128), real),
            pltpu.VMEM((4, 9, 1, cols), real),
            pltpu.VMEM((4, 1, 128), real),
            pltpu.VMEM((25, tall, 128), real),
            pltpu.VMEM((group, 5, 2, tall, 128), real),
            pltpu.VMEM((lines, group * cols, 256), half),
            pltpu.VMEM((lines, group * cols, 256), half),
            pltpu.VMEM((edge_cells, 128), real),
            *work,
            pltpu.SemaphoreType.DMA(()),
            pltpu.SemaphoreType.DMA((lines,)),
            pltpu.SemaphoreType.DMA((2, 4)),
            pltpu.SemaphoreType.DMA((2, 2, 4)),
            pltpu.SemaphoreType.DMA((2, 2, PARTS + 2)),
            pltpu.SemaphoreType.DMA((2, 4, 4)),
        ],
        compiler_params=pltpu.CompilerParams(
            collective_id=0, has_side_effects=True, vmem_limit_bytes=44 * 2**20
        ),
    )(*[pltpu.with_memory_space_constraint(a, pltpu.HBM) for a in (coefficients, vectors)])
    steps = width // STEP
    image, normal = pl.pallas_call(
        write_kernel,
        out_shape=(
            jax.ShapeDtypeStruct(vectors.shape, real),
            jax.ShapeDtypeStruct((25, rows, cols), real),
        ),
        in_specs=[vmem] * 7,
        out_specs=(hbm, hbm),
        scratch_shapes=[
            pltpu.VMEM((steps, 2, 2, cols - 2 * EDGE, STEP), real),
            pltpu.VMEM((steps, rows, 2 * EDGE, STEP), real),
            *work,
            pltpu.SemaphoreType.DMA((2 + lines + 4 * steps,)),
        ],
        compiler_params=pltpu.CompilerParams(vmem_limit_bytes=8 * 2**20),
    )(*[pltpu.with_memory_space_constraint(a, pltpu.VMEM) for a in found])
    return (normal, image)


def solution(mesh):
    in_specs = (P(None, "gy", "gx"), P("gy", "gx", None))
    out_specs = (P(None, "gy", "gx"), P("gy", "gx", None))
    return jax.shard_map(
        per_device, mesh=mesh, in_specs=in_specs, out_specs=out_specs, check_vma=False
    )
```

```python
import functools
import jax
import jax.numpy as jnp
from jax import lax
from jax.experimental import pallas as pl
from jax.experimental.pallas import tpu as pltpu
from jax.sharding import PartitionSpec as P

MESH = pl.DeviceIdType.MESH
PARTS = 2
STEP = 512
EARLY = 512
ROWWAYS = ((1, 0), (-1, 0))
COLWAYS = ((0, 1), (0, -1))
FORWARD = ((1, 0), (0, 1))
CORNERS = ((1, 1), (1, -1), (-1, 1), (-1, -1))
EDGE = 8


def slot_of(e, f):
    return (e + 2) * 5 + (f + 2)


def two(value):
    top = value.astype(jnp.bfloat16).astype(jnp.float32)
    return top, value - top


def dot(a, b):
    return jnp.dot(a, b, preferred_element_type=jnp.float32)


def row_terms(halo, band, xrow):
    depth = halo.shape[0] * halo.shape[1]
    top, rest = two(halo.reshape(depth, halo.shape[2]))
    xrow[0:depth] = top.astype(jnp.bfloat16)
    xrow[depth : 2 * depth] = rest.astype(jnp.bfloat16)
    xrow[2 * depth : 3 * depth] = top.astype(jnp.bfloat16)
    return dot(band[...], xrow[...]).reshape(halo.shape)


def gather_side(side, part, xs):
    def gather(r, carry):
        raw = side[pl.ds(r * 4, 4), :, part]
        near = lax.broadcasted_iota(jnp.int32, raw.shape, 1) < 4
        top, rest = two(jnp.where(near, raw, 0.0))
        both = jnp.concatenate([top[:, 0:4], rest[:, 0:4], top], axis=1)
        xs[pl.ds(r * 4, 4)] = both.astype(jnp.bfloat16)
        return carry

    lax.fori_loop(0, side.shape[0] // 4, gather, 0)


def side_terms(g, group, side_band, xs):
    width = xs.shape[2]
    s = xs[pl.ds(g * group, 2 * group)].reshape(2 * group * 16, width)
    count = group * 2 * EDGE
    total = dot(side_band[g * count : (g + 1) * count, :], s)
    return total.reshape(group, 2 * EDGE, width)


def main_kernel(ny, nx, coef_hbm, x_hbm, *refs):
    (
        image, normal, up, down, side, row_band, side_band,
        coef, xbuf, xh, xl, weights, strips, ring, edges, corners, bends, norm,
        sources, high, low, side_raw, xrow, xs,
        greeting, coef_sem, load_sem, strip_sems, row_sems, col_sems, relay_sems,
    ) = refs
    rows, cols, lanes = x_hbm.shape
    group = 128 // cols
    lines = rows // group
    tall = weights.shape[1]
    tiles = 2
    width = lanes // PARTS
    gy = lax.axis_index("gy")
    gx = lax.axis_index("gx")

    def there(dy, dx):
        y = gy + dy
        x = gx + dx
        return (y >= 0) & (y < ny) & (x >= 0) & (x < nx)

    barrier = pltpu.get_barrier_semaphore()
    count = jnp.int32(0)
    for dy, dx in FORWARD:
        count = count + there(-dy, -dx).astype(jnp.int32)

        @pl.when(there(dy, dx))
        def _():
            pl.semaphore_signal(barrier, inc=1, device_id={"gy": gy + dy, "gx": gx + dx}, device_id_type=MESH)

    coef_load = pltpu.make_async_copy(coef_hbm, coef, coef_sem)
    coef_load.start()
    loads = []
    for g in range(lines):
        at = pl.ds(g * group, group)
        loads.append(pltpu.make_async_copy(x_hbm.at[at], xbuf.at[at], load_sem.at[g]))
    for g in (0, lines - 1):
        loads[g].start()

    def job(send, arrive, source, target, dy, dx, sems, *slot):
        copy = pltpu.make_async_remote_copy(
            source, target, sems.at[(0, *slot)], sems.at[(1, *slot)],
            device_id={"gy": gy + dy, "gx": gx + dx}, device_id_type=MESH,
        )
        return send, arrive, copy

    def start(jobs):
        for send, _, copy in jobs:

            @pl.when(send)
            def _():
                copy.start()

    def await_greeting(n):
        @pl.when(there(*FORWARD[n]))
        def _():
            pl.semaphore_wait(greeting.at[n], 1)

    def arrived(jobs):
        for _, arrive, copy in jobs:

            @pl.when(arrive)
            def _():
                copy.wait_recv()

    mine = {1: pl.ds(rows - 2, 2), -1: pl.ds(0, 2)}
    held = {1: pl.ds(rows, 2), -1: pl.ds(2, 2)}
    land = {1: pl.ds(0, 2), -1: pl.ds(rows + 2, 2)}
    spot = {1: pl.ds(0, 2), -1: pl.ds(2, 2)}
    last = {1: pl.ds(cols - 2, 2), -1: pl.ds(0, 2)}
    odd = gx % 2
    early = EARLY
    near = pl.ds(pl.multiple_of((1 - odd) * (cols - EDGE), EDGE), EDGE)
    far = pl.ds(pl.multiple_of(odd * EDGE, EDGE), cols - EDGE)
    row_strips, col_strips, row_near, row_far, col_ends, col_bulk = [], [], [], [[], [], []], [], [[], []]
    for n, (dy, dx) in enumerate(ROWWAYS):
        send, arrive = there(dy, dx), there(-dy, -dx)
        halo = up if dy > 0 else down
        row_strips.append(job(
            send, arrive, coef_hbm.at[:, pl.ds(rows - 1 if dy > 0 else 0, 1)], ring.at[n], dy, dx, strip_sems, n
        ))
        row_near.append(job(
            send, arrive, x_hbm.at[mine[dy], near], halo.at[:, near], dy, dx, row_sems, n, 0
        ))
        for m, (begin, size) in enumerate(((0, early), (early, width - early), (width, lanes - width))):
            part = pl.ds(begin, size)
            row_far[m].append(job(
                send, arrive, x_hbm.at[mine[dy], far, part], halo.at[:, far, part], dy, dx, row_sems, n, m + 1
            ))
    for n, (dy, dx) in enumerate(COLWAYS):
        send, arrive = there(dy, dx), there(-dy, -dx)
        col_strips.append(job(send, arrive, strips.at[n], edges.at[n], dy, dx, strip_sems, n + 2))
        for m, way in enumerate((1, -1)):
            col_ends.append(job(
                send, arrive, x_hbm.at[mine[way], last[dx]], side.at[held[way], spot[dx]], dy, dx, col_sems, n, m
            ))
        for m in range(PARTS):
            part = pl.ds(m * width, width)
            col_bulk[m].append(job(
                send, arrive, x_hbm.at[pl.ds(2, rows - 4), last[dx], part],
                side.at[pl.ds(4, rows - 4), spot[dx], part], dy, dx, col_sems, n, m + 2
            ))
    turn_x, turn_y, corner_x, corner_y = [], [], [], []
    for n, (dy, dx) in enumerate(CORNERS):
        carrier = odd == (0 if dx > 0 else 1)
        by_x = carrier & there(-dy, 0) & there(0, dx)
        by_y = carrier & there(0, -dx) & there(dy, 0)
        whole = there(-dy, -dx)
        from_x = whole & jnp.logical_not(carrier)
        from_y = whole & carrier
        halo = up if dy > 0 else down
        target = side.at[land[dy], spot[dx]]
        turn_x.append(job(by_x, from_x, halo.at[:, last[dx]], target, 0, dx, relay_sems, n, 0))
        turn_y.append(job(by_y, from_y, side.at[held[dy], spot[dx]], target, dy, 0, relay_sems, n, 1))
        corner_x.append(job(
            by_x, from_x, ring.at[0 if dy > 0 else 1], corners.at[n], 0, dx, relay_sems, n, 2
        ))
        source = edges.at[0 if dx > 0 else 1, pl.ds(lines if dy > 0 else 0, 1)]
        corner_y.append(job(by_y, from_y, source, bends.at[n], dy, 0, relay_sems, n, 3))

    dense = (tall, 128)
    line = lax.broadcasted_iota(jnp.int32, dense, 0)
    lane = lax.broadcasted_iota(jnp.int32, dense, 1)
    place = lane // cols
    column = lane % cols
    row_pos = gy * rows + group * line - 2 + place

    @pl.when(count > 0)
    def _():
        pl.semaphore_wait(barrier, count)

    for n, (dy, dx) in enumerate(FORWARD):

        @pl.when(there(-dy, -dx))
        def _():
            pl.semaphore_signal(
                greeting.at[n], inc=1, device_id={"gy": gy - dy, "gx": gx - dx}, device_id_type=MESH
            )

    start([row_strips[1], row_near[1], row_far[0][1], *col_ends[2:4]])
    coef_load.wait()
    weights[...] = jnp.zeros_like(weights)
    first = [((i - 2) % group, 0 if i >= 2 else 1) for i in range(group)]
    for k in range(9):
        for i, (row, h) in enumerate(first):
            weights[k, pl.ds(h, lines), i * cols : (i + 1) * cols] = coef[k, pl.ds(row, lines, stride=group), :]
    for s in range(2):
        strip = jnp.zeros(dense, jnp.float32)
        for k in range(9):
            moved = pltpu.roll(weights[k], (k - (cols - 1) * (1 - s)) % 128, 1)
            strip = jnp.where(column == k, moved, strip)
        strips[s] = strip

    for load in loads[1 : lines - 1]:
        load.start()
    start([col_strips[1], col_bulk[0][1], col_bulk[1][1]])
    await_greeting(0)
    start([row_strips[0], row_near[0], row_far[0][0]])
    await_greeting(1)
    start([*col_ends[0:2], col_strips[0], col_bulk[0][0], col_bulk[1][0]])
    loads[0].wait()
    loads[lines - 1].wait()

    for target, dy in ((up, 1), (down, -1)):

        @pl.when(jnp.logical_not(there(-dy, 0)))
        def _():
            target[...] = jnp.zeros_like(target)

    for dx in (1, -1):

        @pl.when(jnp.logical_not(there(0, -dx)))
        def _():
            side[2 : rows + 2, spot[dx]] = jnp.zeros((rows, 2, lanes), jnp.float32)

        for dy in (1, -1):

            @pl.when(jnp.logical_not(there(-dy, -dx)))
            def _():
                side[land[dy], spot[dx]] = jnp.zeros((2, 2, lanes), jnp.float32)

    blank = jnp.zeros((2,) + xh.shape[1:], jnp.bfloat16)
    for ref in (xh, xl):
        ref[0:2] = blank
        ref[rows + 2 : rows + 4] = blank

    for g in (0, lines - 1, *range(1, lines - 1)):
        if 0 < g < lines - 1:
            loads[g].wait()

        def split(n, carry):
            part = pl.ds(pl.multiple_of(n * STEP, STEP), STEP)
            top, rest = two(xbuf[g * group : (g + 1) * group, :, part])
            xh[g * group + 2 : (g + 1) * group + 2, :, part] = top.astype(jnp.bfloat16)
            xl[g * group + 2 : (g + 1) * group + 2, :, part] = rest.astype(jnp.bfloat16)
            return carry

        lax.fori_loop(0, lanes // STEP, split, 0)

    arrived(col_strips + col_ends)
    start(corner_y + turn_y + row_far[1] + row_far[2])
    arrived(row_strips)
    start(corner_x)

    def inside(a, b, col_pos):
        row = row_pos + a
        col = col_pos + b
        return (row >= 0) & (row < ny * rows) & (col >= 0) & (col < nx * cols)

    def down_rows(value, a):
        if a == 0:
            return value
        moved = pltpu.roll(value, (a * cols) % 128, 1)
        crossed = pltpu.roll(moved, a % tall, 0)
        return jnp.where(place == (0 if a > 0 else group - 1), crossed, moved)

    def assemble(sides):
        col_pos = gx * cols + column
        kept = []
        for k in range(9):
            a = k // 3 - 1
            b = k % 3 - 1
            own = jnp.where(inside(a, b, col_pos), weights[k], 0.0)
            before = pltpu.roll(sides[0], (-k) % 128, 1)
            before = jnp.where(inside(a, b, gx * cols - 1), before, 0.0)
            after = pltpu.roll(sides[1], (cols - 1 - k) % 128, 1)
            after = jnp.where(inside(a, b, (gx + 1) * cols), after, 0.0)
            right = jnp.where(column == 0, before, pltpu.roll(own, 1, 1))
            left = jnp.where(column == cols - 1, after, pltpu.roll(own, 127, 1))
            kept.append((left, own, right))
        terms = [None] * 25
        for k in range(9):
            a = k // 3 - 1
            b = k % 3 - 1
            moved = [down_rows(kept[m][b + 1], a) for m in range(9)]
            for m in range(9):
                slot = slot_of(m // 3 - k // 3, m % 3 - k % 3)
                product = moved[k] * moved[m]
                terms[slot] = product if terms[slot] is None else terms[slot] + product
        for slot in range(25):
            norm[slot] = terms[slot]

        for rr in range(group):
            for f in range(-2, 3):
                for t in range(tiles):
                    total = jnp.zeros(dense, jnp.float32)
                    for i in range(group):
                        e = t * group + i - 2 - rr
                        if -2 <= e <= 2:
                            total = jnp.where(place == i, norm[slot_of(-e, -f)], total)
                    sources[rr, f + 2, t] = total

    shape = (cols, 128)
    lane_b = lax.broadcasted_iota(jnp.int32, shape, 1)
    offset = lane_b % cols - lax.broadcasted_iota(jnp.int32, shape, 0)

    def band(g, rr, t):
        total = jnp.zeros(shape, jnp.float32)
        for f in range(-2, 3):
            source = sources[rr, f + 2, t, pl.ds(g + t, 1), :]
            total = jnp.where(offset == f, jnp.broadcast_to(source, shape), total)
        return total

    def build(g, carry):
        for rr in range(group):
            for t in range(tiles):
                top, rest = two(band(g, rr, t))
                at = (g, pl.ds(rr * cols, cols), pl.ds(t * 128, 128))
                high[at] = top.astype(jnp.bfloat16)
                low[at] = rest.astype(jnp.bfloat16)
        return carry


    def local(groups):
        def body(n, carry):
            part = pl.ds(pl.multiple_of(n * STEP, STEP), STEP)
            for g in groups:
                span = pl.ds(g * group, 2 * group)
                h = xh[span, :, part].reshape(2 * group * cols, STEP)
                l = xl[span, :, part].reshape(2 * group * cols, STEP)
                total = dot(high[g], h) + dot(low[g], h) + dot(high[g], l)
                image[pl.ds(g * group, group), :, part] = total.reshape(group, cols, STEP)
            return carry

        return body

    sides = [jnp.where(there(0, -dx), edges[n], 0.0) for n, (_, dx) in enumerate(COLWAYS)]
    assemble(sides)
    lax.fori_loop(1, lines - 1, build, 0)
    inner = range(1, lines - 1)
    lax.fori_loop(0, 2, local(inner), 0)
    arrived(row_near)
    start(turn_x)
    lax.fori_loop(2, lanes // STEP, local(inner), 0)
    arrived(corner_y + corner_x)


    ring_place = {1: (0, 1), -1: (lines, 2)}
    for n, (dy, dx) in enumerate(ROWWAYS):
        h, i = ring_place[dy]
        for k in range(9):
            weights[k, pl.ds(h, 1), i * cols : (i + 1) * cols] = jnp.where(there(-dy, -dx), ring[n, k], 0.0)
    for n, (dy, dx) in enumerate(CORNERS):
        h, i = ring_place[dy]
        here = (line == h) & (place == i)
        at = cols - 1 if dx > 0 else 0
        straight = jnp.zeros(dense, jnp.float32)
        for k in range(9):
            value = jnp.broadcast_to(corners[n, k][:, at : at + 1], dense)
            straight = jnp.where(column == k, value, straight)
        carrier = odd == (0 if dx > 0 else 1)
        value = jnp.where(carrier, jnp.broadcast_to(bends[n], dense), straight)
        value = jnp.where(there(-dy, -dx), value, 0.0)
        s = 0 if dx > 0 else 1
        sides[s] = jnp.where(here, value, sides[s])

    assemble(sides)
    for g in (0, lines - 1):
        build(g, 0)
    lax.fori_loop(0, lanes // STEP, local((0, lines - 1)), 0)

    depth = 2 * cols
    for s in range(2):
        for n in range(2):
            value = band(0, n, 0) if s == 0 else band(lines - 1, group - 2 + n, 1)
            if s:
                value = pltpu.roll(value, 128 - depth, 1)
            top, rest = two(jnp.where(lane_b < depth, value, 0.0))
            at = pl.ds(n * cols, cols)
            row_band[s, at, 0:128] = (top + pltpu.roll(top, depth, 1)).astype(jnp.bfloat16)
            row_band[s, at, 128:256] = rest.astype(jnp.bfloat16)

    side_raw[...] = jnp.zeros_like(side_raw)
    thin = (lines, 128)
    lane_s = lax.broadcasted_iota(jnp.int32, thin, 1)
    pairs = ((0, 0, -2), (0, 1, -1), (1, 1, -2), (cols - 2, 2, 2), (cols - 1, 2, 1), (cols - 1, 3, 2))
    for rr in range(group):
        h = (rr + 2) // group
        i = (rr + 2) % group
        for c in (0, 1, cols - 2, cols - 1):
            total = jnp.zeros(thin, jnp.float32)
            for own, j, f in pairs:
                if own != c:
                    continue
                for e in range(-2, 3):
                    wanted = (lane_s // 16 == rr + 2 + e) & (lane_s % 4 == j) & (lane_s % 16 < 12)
                    at = i * cols + c
                    value = norm[slot_of(e, f), pl.ds(h, lines), :][:, at : at + 1]
                    total = jnp.where(wanted, jnp.broadcast_to(value, thin), total)
            spot = rr * 2 * EDGE + (c if c < 2 else c - cols + 2 * EDGE)
            side_raw[pl.ds(spot, lines, stride=2 * EDGE * group), :] = total
    top, rest = two(side_raw[...])
    part = lax.broadcasted_iota(jnp.int32, side_raw.shape, 1) % 16
    side_band[...] = jnp.where(part < 8, top, rest).astype(jnp.bfloat16)

    def spread(slot, carry):
        for i, (row, h) in enumerate(first):
            value = norm[slot, pl.ds(h, lines), :]
            normal[slot, pl.ds(row, lines, stride=group), :] = value[:, i * cols : (i + 1) * cols]
        return carry

    lax.fori_loop(0, 25, spread, 0, unroll=5)
    xrow[3 * depth : 4 * depth] = jnp.zeros((depth, STEP), jnp.bfloat16)

    arrived(turn_x + turn_y)
    for n in range(PARTS - 1):
        arrived(row_far[0] + row_far[1] + col_bulk[n])

        def beside(m, carry):
            part = pl.ds(pl.multiple_of(n * width + m * STEP, STEP), STEP)
            for s, halo in enumerate((up, down)):
                at = pl.ds(0 if s == 0 else rows - 2, 2)
                total = row_terms(halo[:, :, part], row_band.at[s], xrow)
                image[at, :, part] = image[at, :, part] + total
            gather_side(side, part, xs)
            for g in range(lines):
                total = side_terms(g, group, side_band, xs)
                at = pl.ds(g * group, group)
                image[at, 0:EDGE, part] = image[at, 0:EDGE, part] + total[:, 0:EDGE]
                image[at, cols - EDGE : cols, part] = image[at, cols - EDGE : cols, part] + total[:, EDGE:]
            return carry

        lax.fori_loop(0, width // STEP, beside, 0)
    def sent(jobs):
        for send, _, copy in jobs:

            @pl.when(send)
            def _():
                copy.wait_send()

    sent(row_strips + col_strips + row_near + col_ends + turn_x + turn_y + corner_x + corner_y)
    sent(row_far[0] + row_far[1] + col_bulk[0])
    arrived(col_bulk[PARTS - 1] + row_far[2])
    sent(col_bulk[PARTS - 1] + row_far[2])


def write_kernel(image, normal, up, down, side, row_band, side_band, image_hbm, normal_hbm, *scratch):
    middle, flank, xrow, xs, sem = scratch
    rows, cols, lanes = image.shape
    group = 128 // cols
    lines = rows // group
    width = lanes // PARTS
    head = lanes - width
    depth = 2 * cols
    inner = slice(EDGE, cols - EDGE)
    copies = []

    def send(source, *at):
        copies.append(pltpu.make_async_copy(source, image_hbm.at[at], sem.at[len(copies)]))
        copies[-1].start()

    copies.append(pltpu.make_async_copy(normal, normal_hbm, sem.at[0]))
    copies[0].start()
    for g in range(lines):
        at = pl.ds(g * group, group)
        send(image.at[at, :, 0:head], at, slice(None), pl.ds(0, head))
    at = pl.ds(2, rows - 4)
    send(image.at[at, inner, head:lanes], at, inner, pl.ds(head, width))

    xrow[3 * depth : 4 * depth] = jnp.zeros((depth, STEP), jnp.bfloat16)
    for n in range(width // STEP):
        whole = pl.ds(head + n * STEP, STEP)
        gather_side(side, whole, xs)
        for g in range(lines):
            at = pl.ds(g * group, group)
            total = side_terms(g, group, side_band, xs)
            flank[n, at, 0:EDGE] = image[at, 0:EDGE, whole] + total[:, 0:EDGE]
            flank[n, at, EDGE:] = image[at, cols - EDGE : cols, whole] + total[:, EDGE:]
        for s, halo in enumerate((up, down)):
            at = pl.ds(0 if s == 0 else rows - 2, 2)
            total = row_terms(halo[:, :, whole], row_band.at[s], xrow)
            middle[n, s] = image[at, inner, whole] + total[:, inner]
            flank[n, at, 0:EDGE] = flank[n, at, 0:EDGE] + total[:, 0:EDGE]
            flank[n, at, EDGE:] = flank[n, at, EDGE:] + total[:, cols - EDGE :]
            send(middle.at[n, s], at, inner, whole)
        send(flank.at[n, :, 0:EDGE], slice(None), pl.ds(0, EDGE), whole)
        send(flank.at[n, :, EDGE:], slice(None), pl.ds(cols - EDGE, EDGE), whole)
    for copy in copies:
        copy.wait()


def per_device(coefficients, vectors):
    rows, cols, lanes = vectors.shape
    ny = lax.axis_size("gy")
    nx = lax.axis_size("gx")
    group = 128 // cols
    lines = rows // group
    tall = -(-(lines + 1) // 8) * 8
    width = lanes // PARTS
    edge_cells = lines * group * 2 * EDGE
    real = jnp.float32
    half = jnp.bfloat16
    hbm = pl.BlockSpec(memory_space=pltpu.HBM)
    vmem = pl.BlockSpec(memory_space=pltpu.VMEM)
    work = (pltpu.VMEM((8 * cols, STEP), half), pltpu.VMEM((rows + 4, 16, STEP), half))
    found = pl.pallas_call(
        functools.partial(main_kernel, ny, nx),
        out_shape=(
            pltpu.VMEM(vectors.shape, real),
            pltpu.VMEM((25, rows, cols), real),
            pltpu.VMEM((2, cols, lanes), real),
            pltpu.VMEM((2, cols, lanes), real),
            pltpu.VMEM((rows + 4, 8, lanes), real),
            pltpu.VMEM((2, 2 * cols, 256), half),
            pltpu.VMEM((edge_cells, 128), half),
        ),
        in_specs=[hbm, hbm],
        out_specs=(vmem,) * 7,
        scratch_shapes=[
            pltpu.VMEM((9, rows, cols), real),
            pltpu.VMEM(vectors.shape, real),
            pltpu.VMEM((rows + 4, cols, lanes), half),
            pltpu.VMEM((rows + 4, cols, lanes), half),
            pltpu.VMEM((9, tall, 128), real),
            pltpu.VMEM((2, tall, 128), real),
            pltpu.VMEM((2, 9, 1, cols), real),
            pltpu.VMEM((2, tall, 128), real),
            pltpu.VMEM((4, 9, 1, cols), real),
            pltpu.VMEM((4, 1, 128), real),
            pltpu.VMEM((25, tall, 128), real),
            pltpu.VMEM((group, 5, 2, tall, 128), real),
            pltpu.VMEM((lines, group * cols, 256), half),
            pltpu.VMEM((lines, group * cols, 256), half),
            pltpu.VMEM((edge_cells, 128), real),
            *work,
            pltpu.SemaphoreType.REGULAR((2,)),
            pltpu.SemaphoreType.DMA(()),
            pltpu.SemaphoreType.DMA((lines,)),
            pltpu.SemaphoreType.DMA((2, 4)),
            pltpu.SemaphoreType.DMA((2, 2, 4)),
            pltpu.SemaphoreType.DMA((2, 2, PARTS + 2)),
            pltpu.SemaphoreType.DMA((2, 4, 4)),
        ],
        compiler_params=pltpu.CompilerParams(
            collective_id=0, has_side_effects=True, vmem_limit_bytes=44 * 2**20
        ),
    )(*[pltpu.with_memory_space_constraint(a, pltpu.HBM) for a in (coefficients, vectors)])
    steps = width // STEP
    image, normal = pl.pallas_call(
        write_kernel,
        out_shape=(
            jax.ShapeDtypeStruct(vectors.shape, real),
            jax.ShapeDtypeStruct((25, rows, cols), real),
        ),
        in_specs=[vmem] * 7,
        out_specs=(hbm, hbm),
        scratch_shapes=[
            pltpu.VMEM((steps, 2, 2, cols - 2 * EDGE, STEP), real),
            pltpu.VMEM((steps, rows, 2 * EDGE, STEP), real),
            *work,
            pltpu.SemaphoreType.DMA((2 + lines + 4 * steps,)),
        ],
        compiler_params=pltpu.CompilerParams(vmem_limit_bytes=8 * 2**20),
    )(*[pltpu.with_memory_space_constraint(a, pltpu.VMEM) for a in found])
    return (normal, image)


def solution(mesh):
    in_specs = (P(None, "gy", "gx"), P("gy", "gx", None))
    out_specs = (P(None, "gy", "gx"), P("gy", "gx", None))
    return jax.shard_map(
        per_device, mesh=mesh, in_specs=in_specs, out_specs=out_specs, check_vma=False
    )
```

```python
import functools
import jax
import jax.numpy as jnp
from jax import lax
from jax.experimental import pallas as pl
from jax.experimental.pallas import tpu as pltpu
from jax.sharding import PartitionSpec as P

MESH = pl.DeviceIdType.MESH
PARTS = 2
STEP = 512
EARLY = 640
ROWWAYS = ((1, 0), (-1, 0))
COLWAYS = ((0, 1), (0, -1))
FORWARD = ((1, 0), (0, 1))
CORNERS = ((1, 1), (1, -1), (-1, 1), (-1, -1))
EDGE = 8


def slot_of(e, f):
    return (e + 2) * 5 + (f + 2)


def two(value):
    top = value.astype(jnp.bfloat16).astype(jnp.float32)
    return top, value - top


def dot(a, b):
    return jnp.dot(a, b, preferred_element_type=jnp.float32)


def row_terms(halo, band, xrow):
    depth = halo.shape[0] * halo.shape[1]
    top, rest = two(halo.reshape(depth, halo.shape[2]))
    xrow[0:depth] = top.astype(jnp.bfloat16)
    xrow[depth : 2 * depth] = rest.astype(jnp.bfloat16)
    xrow[2 * depth : 3 * depth] = top.astype(jnp.bfloat16)
    return dot(band[...], xrow[...]).reshape(halo.shape)


def gather_side(side, part, xs):
    def gather(r, carry):
        raw = side[pl.ds(r * 4, 4), :, part]
        near = lax.broadcasted_iota(jnp.int32, raw.shape, 1) < 4
        top, rest = two(jnp.where(near, raw, 0.0))
        both = jnp.concatenate([top[:, 0:4], rest[:, 0:4], top], axis=1)
        xs[pl.ds(r * 4, 4)] = both.astype(jnp.bfloat16)
        return carry

    lax.fori_loop(0, side.shape[0] // 4, gather, 0)


def side_terms(g, group, side_band, xs):
    width = xs.shape[2]
    s = xs[pl.ds(g * group, 2 * group)].reshape(2 * group * 16, width)
    count = group * 2 * EDGE
    total = dot(side_band[g * count : (g + 1) * count, :], s)
    return total.reshape(group, 2 * EDGE, width)


def main_kernel(ny, nx, coef_hbm, x_hbm, *refs):
    (
        image, normal, up, down, side, row_band, side_band,
        coef, xbuf, xh, xl, weights, strips, ring, edges, corners, bends, norm,
        sources, high, low, side_raw, xrow, xs,
        greeting, coef_sem, load_sem, strip_sems, row_sems, col_sems, relay_sems,
    ) = refs
    rows, cols, lanes = x_hbm.shape
    group = 128 // cols
    lines = rows // group
    tall = weights.shape[1]
    tiles = 2
    width = lanes // PARTS
    gy = lax.axis_index("gy")
    gx = lax.axis_index("gx")

    def there(dy, dx):
        y = gy + dy
        x = gx + dx
        return (y >= 0) & (y < ny) & (x >= 0) & (x < nx)

    barrier = pltpu.get_barrier_semaphore()
    count = jnp.int32(0)
    for dy, dx in FORWARD:
        count = count + there(-dy, -dx).astype(jnp.int32)

        @pl.when(there(dy, dx))
        def _():
            pl.semaphore_signal(barrier, inc=1, device_id={"gy": gy + dy, "gx": gx + dx}, device_id_type=MESH)

    coef_load = pltpu.make_async_copy(coef_hbm, coef, coef_sem)
    coef_load.start()
    loads = []
    for g in range(lines):
        at = pl.ds(g * group, group)
        loads.append(pltpu.make_async_copy(x_hbm.at[at], xbuf.at[at], load_sem.at[g]))
    for g in (0, lines - 1):
        loads[g].start()

    def job(send, arrive, source, target, dy, dx, sems, *slot):
        copy = pltpu.make_async_remote_copy(
            source, target, sems.at[(0, *slot)], sems.at[(1, *slot)],
            device_id={"gy": gy + dy, "gx": gx + dx}, device_id_type=MESH,
        )
        return send, arrive, copy

    def start(jobs):
        for send, _, copy in jobs:

            @pl.when(send)
            def _():
                copy.start()

    def await_greeting(n):
        @pl.when(there(*FORWARD[n]))
        def _():
            pl.semaphore_wait(greeting.at[n], 1)

    def arrived(jobs):
        for _, arrive, copy in jobs:

            @pl.when(arrive)
            def _():
                copy.wait_recv()

    mine = {1: pl.ds(rows - 2, 2), -1: pl.ds(0, 2)}
    held = {1: pl.ds(rows, 2), -1: pl.ds(2, 2)}
    land = {1: pl.ds(0, 2), -1: pl.ds(rows + 2, 2)}
    spot = {1: pl.ds(0, 2), -1: pl.ds(2, 2)}
    last = {1: pl.ds(cols - 2, 2), -1: pl.ds(0, 2)}
    odd = gx % 2
    early = EARLY
    near = pl.ds(pl.multiple_of((1 - odd) * (cols - EDGE), EDGE), EDGE)
    far = pl.ds(pl.multiple_of(odd * EDGE, EDGE), cols - EDGE)
    row_strips, col_strips, row_near, row_far, col_ends, col_bulk = [], [], [], [[], [], []], [], [[], []]
    for n, (dy, dx) in enumerate(ROWWAYS):
        send, arrive = there(dy, dx), there(-dy, -dx)
        halo = up if dy > 0 else down
        row_strips.append(job(
            send, arrive, coef_hbm.at[:, pl.ds(rows - 1 if dy > 0 else 0, 1)], ring.at[n], dy, dx, strip_sems, n
        ))
        row_near.append(job(
            send, arrive, x_hbm.at[mine[dy], near], halo.at[:, near], dy, dx, row_sems, n, 0
        ))
        for m, (begin, size) in enumerate(((0, early), (early, width - early), (width, lanes - width))):
            part = pl.ds(begin, size)
            row_far[m].append(job(
                send, arrive, x_hbm.at[mine[dy], far, part], halo.at[:, far, part], dy, dx, row_sems, n, m + 1
            ))
    for n, (dy, dx) in enumerate(COLWAYS):
        send, arrive = there(dy, dx), there(-dy, -dx)
        col_strips.append(job(send, arrive, strips.at[n], edges.at[n], dy, dx, strip_sems, n + 2))
        for m, way in enumerate((1, -1)):
            col_ends.append(job(
                send, arrive, x_hbm.at[mine[way], last[dx]], side.at[held[way], spot[dx]], dy, dx, col_sems, n, m
            ))
        for m in range(PARTS):
            part = pl.ds(m * width, width)
            col_bulk[m].append(job(
                send, arrive, x_hbm.at[pl.ds(2, rows - 4), last[dx], part],
                side.at[pl.ds(4, rows - 4), spot[dx], part], dy, dx, col_sems, n, m + 2
            ))
    turn_x, turn_y, corner_x, corner_y = [], [], [], []
    for n, (dy, dx) in enumerate(CORNERS):
        carrier = odd == (0 if dx > 0 else 1)
        by_x = carrier & there(-dy, 0) & there(0, dx)
        by_y = carrier & there(0, -dx) & there(dy, 0)
        whole = there(-dy, -dx)
        from_x = whole & jnp.logical_not(carrier)
        from_y = whole & carrier
        halo = up if dy > 0 else down
        target = side.at[land[dy], spot[dx]]
        turn_x.append(job(by_x, from_x, halo.at[:, last[dx]], target, 0, dx, relay_sems, n, 0))
        turn_y.append(job(by_y, from_y, side.at[held[dy], spot[dx]], target, dy, 0, relay_sems, n, 1))
        corner_x.append(job(
            by_x, from_x, ring.at[0 if dy > 0 else 1], corners.at[n], 0, dx, relay_sems, n, 2
        ))
        source = edges.at[0 if dx > 0 else 1, pl.ds(lines if dy > 0 else 0, 1)]
        corner_y.append(job(by_y, from_y, source, bends.at[n], dy, 0, relay_sems, n, 3))

    dense = (tall, 128)
    line = lax.broadcasted_iota(jnp.int32, dense, 0)
    lane = lax.broadcasted_iota(jnp.int32, dense, 1)
    place = lane // cols
    column = lane % cols
    row_pos = gy * rows + group * line - 2 + place

    @pl.when(count > 0)
    def _():
        pl.semaphore_wait(barrier, count)

    for n, (dy, dx) in enumerate(FORWARD):

        @pl.when(there(-dy, -dx))
        def _():
            pl.semaphore_signal(
                greeting.at[n], inc=1, device_id={"gy": gy - dy, "gx": gx - dx}, device_id_type=MESH
            )

    start([row_strips[1], row_near[1], row_far[0][1], *col_ends[2:4]])
    coef_load.wait()
    weights[...] = jnp.zeros_like(weights)
    first = [((i - 2) % group, 0 if i >= 2 else 1) for i in range(group)]
    for k in range(9):
        for i, (row, h) in enumerate(first):
            weights[k, pl.ds(h, lines), i * cols : (i + 1) * cols] = coef[k, pl.ds(row, lines, stride=group), :]
    for s in range(2):
        strip = jnp.zeros(dense, jnp.float32)
        for k in range(9):
            moved = pltpu.roll(weights[k], (k - (cols - 1) * (1 - s)) % 128, 1)
            strip = jnp.where(column == k, moved, strip)
        strips[s] = strip

    for load in loads[1 : lines - 1]:
        load.start()
    start([col_strips[1], col_bulk[0][1], col_bulk[1][1]])
    await_greeting(0)
    start([row_strips[0], row_near[0], row_far[0][0]])
    await_greeting(1)
    start([*col_ends[0:2], col_strips[0], col_bulk[0][0], col_bulk[1][0]])
    loads[0].wait()
    loads[lines - 1].wait()

    for target, dy in ((up, 1), (down, -1)):

        @pl.when(jnp.logical_not(there(-dy, 0)))
        def _():
            target[...] = jnp.zeros_like(target)

    for dx in (1, -1):

        @pl.when(jnp.logical_not(there(0, -dx)))
        def _():
            side[2 : rows + 2, spot[dx]] = jnp.zeros((rows, 2, lanes), jnp.float32)

        for dy in (1, -1):

            @pl.when(jnp.logical_not(there(-dy, -dx)))
            def _():
                side[land[dy], spot[dx]] = jnp.zeros((2, 2, lanes), jnp.float32)

    blank = jnp.zeros((2,) + xh.shape[1:], jnp.bfloat16)
    for ref in (xh, xl):
        ref[0:2] = blank
        ref[rows + 2 : rows + 4] = blank

    for g in (0, lines - 1, *range(1, lines // 2)):
        if 0 < g < lines - 1:
            loads[g].wait()

        def split(n, carry):
            part = pl.ds(pl.multiple_of(n * STEP, STEP), STEP)
            top, rest = two(xbuf[g * group : (g + 1) * group, :, part])
            xh[g * group + 2 : (g + 1) * group + 2, :, part] = top.astype(jnp.bfloat16)
            xl[g * group + 2 : (g + 1) * group + 2, :, part] = rest.astype(jnp.bfloat16)
            return carry

        lax.fori_loop(0, lanes // STEP, split, 0)

    arrived(col_strips + col_ends)
    start(corner_y + turn_y + row_far[1] + row_far[2])
    arrived(row_strips)
    start(corner_x)

    for g in range(lines // 2, lines - 1):
        if 0 < g < lines - 1:
            loads[g].wait()

        def split(n, carry):
            part = pl.ds(pl.multiple_of(n * STEP, STEP), STEP)
            top, rest = two(xbuf[g * group : (g + 1) * group, :, part])
            xh[g * group + 2 : (g + 1) * group + 2, :, part] = top.astype(jnp.bfloat16)
            xl[g * group + 2 : (g + 1) * group + 2, :, part] = rest.astype(jnp.bfloat16)
            return carry

        lax.fori_loop(0, lanes // STEP, split, 0)


    def inside(a, b, col_pos):
        row = row_pos + a
        col = col_pos + b
        return (row >= 0) & (row < ny * rows) & (col >= 0) & (col < nx * cols)

    def down_rows(value, a):
        if a == 0:
            return value
        moved = pltpu.roll(value, (a * cols) % 128, 1)
        crossed = pltpu.roll(moved, a % tall, 0)
        return jnp.where(place == (0 if a > 0 else group - 1), crossed, moved)

    def assemble(sides):
        col_pos = gx * cols + column
        kept = []
        for k in range(9):
            a = k // 3 - 1
            b = k % 3 - 1
            own = jnp.where(inside(a, b, col_pos), weights[k], 0.0)
            before = pltpu.roll(sides[0], (-k) % 128, 1)
            before = jnp.where(inside(a, b, gx * cols - 1), before, 0.0)
            after = pltpu.roll(sides[1], (cols - 1 - k) % 128, 1)
            after = jnp.where(inside(a, b, (gx + 1) * cols), after, 0.0)
            right = jnp.where(column == 0, before, pltpu.roll(own, 1, 1))
            left = jnp.where(column == cols - 1, after, pltpu.roll(own, 127, 1))
            kept.append((left, own, right))
        terms = [None] * 25
        for k in range(9):
            a = k // 3 - 1
            b = k % 3 - 1
            moved = [down_rows(kept[m][b + 1], a) for m in range(9)]
            for m in range(9):
                slot = slot_of(m // 3 - k // 3, m % 3 - k % 3)
                product = moved[k] * moved[m]
                terms[slot] = product if terms[slot] is None else terms[slot] + product
        for slot in range(25):
            norm[slot] = terms[slot]

        for rr in range(group):
            for f in range(-2, 3):
                for t in range(tiles):
                    total = jnp.zeros(dense, jnp.float32)
                    for i in range(group):
                        e = t * group + i - 2 - rr
                        if -2 <= e <= 2:
                            total = jnp.where(place == i, norm[slot_of(-e, -f)], total)
                    sources[rr, f + 2, t] = total

    shape = (cols, 128)
    lane_b = lax.broadcasted_iota(jnp.int32, shape, 1)
    offset = lane_b % cols - lax.broadcasted_iota(jnp.int32, shape, 0)

    def band(g, rr, t):
        total = jnp.zeros(shape, jnp.float32)
        for f in range(-2, 3):
            source = sources[rr, f + 2, t, pl.ds(g + t, 1), :]
            total = jnp.where(offset == f, jnp.broadcast_to(source, shape), total)
        return total

    def build(g, carry):
        for rr in range(group):
            for t in range(tiles):
                top, rest = two(band(g, rr, t))
                at = (g, pl.ds(rr * cols, cols), pl.ds(t * 128, 128))
                high[at] = top.astype(jnp.bfloat16)
                low[at] = rest.astype(jnp.bfloat16)
        return carry


    def local(groups):
        def body(n, carry):
            part = pl.ds(pl.multiple_of(n * STEP, STEP), STEP)
            for g in groups:
                span = pl.ds(g * group, 2 * group)
                h = xh[span, :, part].reshape(2 * group * cols, STEP)
                l = xl[span, :, part].reshape(2 * group * cols, STEP)
                total = dot(high[g], h) + dot(low[g], h) + dot(high[g], l)
                image[pl.ds(g * group, group), :, part] = total.reshape(group, cols, STEP)
            return carry

        return body

    sides = [jnp.where(there(0, -dx), edges[n], 0.0) for n, (_, dx) in enumerate(COLWAYS)]
    assemble(sides)
    lax.fori_loop(1, lines - 1, build, 0)
    inner = range(1, lines - 1)
    lax.fori_loop(0, 2, local(inner), 0)
    arrived(row_near)
    start(turn_x)
    lax.fori_loop(2, lanes // STEP, local(inner), 0)
    arrived(corner_y + corner_x)


    ring_place = {1: (0, 1), -1: (lines, 2)}
    for n, (dy, dx) in enumerate(ROWWAYS):
        h, i = ring_place[dy]
        for k in range(9):
            weights[k, pl.ds(h, 1), i * cols : (i + 1) * cols] = jnp.where(there(-dy, -dx), ring[n, k], 0.0)
    for n, (dy, dx) in enumerate(CORNERS):
        h, i = ring_place[dy]
        here = (line == h) & (place == i)
        at = cols - 1 if dx > 0 else 0
        straight = jnp.zeros(dense, jnp.float32)
        for k in range(9):
            value = jnp.broadcast_to(corners[n, k][:, at : at + 1], dense)
            straight = jnp.where(column == k, value, straight)
        carrier = odd == (0 if dx > 0 else 1)
        value = jnp.where(carrier, jnp.broadcast_to(bends[n], dense), straight)
        value = jnp.where(there(-dy, -dx), value, 0.0)
        s = 0 if dx > 0 else 1
        sides[s] = jnp.where(here, value, sides[s])

    assemble(sides)
    for g in (0, lines - 1):
        build(g, 0)
    lax.fori_loop(0, lanes // STEP, local((0, lines - 1)), 0)

    depth = 2 * cols
    for s in range(2):
        for n in range(2):
            value = band(0, n, 0) if s == 0 else band(lines - 1, group - 2 + n, 1)
            if s:
                value = pltpu.roll(value, 128 - depth, 1)
            top, rest = two(jnp.where(lane_b < depth, value, 0.0))
            at = pl.ds(n * cols, cols)
            row_band[s, at, 0:128] = (top + pltpu.roll(top, depth, 1)).astype(jnp.bfloat16)
            row_band[s, at, 128:256] = rest.astype(jnp.bfloat16)

    side_raw[...] = jnp.zeros_like(side_raw)
    thin = (lines, 128)
    lane_s = lax.broadcasted_iota(jnp.int32, thin, 1)
    pairs = ((0, 0, -2), (0, 1, -1), (1, 1, -2), (cols - 2, 2, 2), (cols - 1, 2, 1), (cols - 1, 3, 2))
    for rr in range(group):
        h = (rr + 2) // group
        i = (rr + 2) % group
        for c in (0, 1, cols - 2, cols - 1):
            total = jnp.zeros(thin, jnp.float32)
            for own, j, f in pairs:
                if own != c:
                    continue
                for e in range(-2, 3):
                    wanted = (lane_s // 16 == rr + 2 + e) & (lane_s % 4 == j) & (lane_s % 16 < 12)
                    at = i * cols + c
                    value = norm[slot_of(e, f), pl.ds(h, lines), :][:, at : at + 1]
                    total = jnp.where(wanted, jnp.broadcast_to(value, thin), total)
            spot = rr * 2 * EDGE + (c if c < 2 else c - cols + 2 * EDGE)
            side_raw[pl.ds(spot, lines, stride=2 * EDGE * group), :] = total
    top, rest = two(side_raw[...])
    part = lax.broadcasted_iota(jnp.int32, side_raw.shape, 1) % 16
    side_band[...] = jnp.where(part < 8, top, rest).astype(jnp.bfloat16)

    def spread(slot, carry):
        for i, (row, h) in enumerate(first):
            value = norm[slot, pl.ds(h, lines), :]
            normal[slot, pl.ds(row, lines, stride=group), :] = value[:, i * cols : (i + 1) * cols]
        return carry

    lax.fori_loop(0, 25, spread, 0, unroll=5)
    xrow[3 * depth : 4 * depth] = jnp.zeros((depth, STEP), jnp.bfloat16)

    arrived(turn_x + turn_y)
    for n in range(PARTS - 1):
        arrived(row_far[0] + row_far[1] + col_bulk[n])

        def beside(m, carry):
            part = pl.ds(pl.multiple_of(n * width + m * STEP, STEP), STEP)
            for s, halo in enumerate((up, down)):
                at = pl.ds(0 if s == 0 else rows - 2, 2)
                total = row_terms(halo[:, :, part], row_band.at[s], xrow)
                image[at, :, part] = image[at, :, part] + total
            gather_side(side, part, xs)
            for g in range(lines):
                total = side_terms(g, group, side_band, xs)
                at = pl.ds(g * group, group)
                image[at, 0:EDGE, part] = image[at, 0:EDGE, part] + total[:, 0:EDGE]
                image[at, cols - EDGE : cols, part] = image[at, cols - EDGE : cols, part] + total[:, EDGE:]
            return carry

        lax.fori_loop(0, width // STEP, beside, 0)
    def sent(jobs):
        for send, _, copy in jobs:

            @pl.when(send)
            def _():
                copy.wait_send()

    sent(row_strips + col_strips + row_near + col_ends + turn_x + turn_y + corner_x + corner_y)
    sent(row_far[0] + row_far[1] + col_bulk[0])
    arrived(col_bulk[PARTS - 1] + row_far[2])
    sent(col_bulk[PARTS - 1] + row_far[2])


def write_kernel(image, normal, up, down, side, row_band, side_band, image_hbm, normal_hbm, *scratch):
    middle, flank, xrow, xs, sem = scratch
    rows, cols, lanes = image.shape
    group = 128 // cols
    lines = rows // group
    width = lanes // PARTS
    head = lanes - width
    depth = 2 * cols
    inner = slice(EDGE, cols - EDGE)
    copies = []

    def send(source, *at):
        copies.append(pltpu.make_async_copy(source, image_hbm.at[at], sem.at[len(copies)]))
        copies[-1].start()

    copies.append(pltpu.make_async_copy(normal, normal_hbm, sem.at[0]))
    copies[0].start()
    for g in range(lines):
        at = pl.ds(g * group, group)
        send(image.at[at, :, 0:head], at, slice(None), pl.ds(0, head))
    at = pl.ds(2, rows - 4)
    send(image.at[at, inner, head:lanes], at, inner, pl.ds(head, width))

    xrow[3 * depth : 4 * depth] = jnp.zeros((depth, STEP), jnp.bfloat16)
    for n in range(width // STEP):
        whole = pl.ds(head + n * STEP, STEP)
        gather_side(side, whole, xs)
        for g in range(lines):
            at = pl.ds(g * group, group)
            total = side_terms(g, group, side_band, xs)
            flank[n, at, 0:EDGE] = image[at, 0:EDGE, whole] + total[:, 0:EDGE]
            flank[n, at, EDGE:] = image[at, cols - EDGE : cols, whole] + total[:, EDGE:]
        for s, halo in enumerate((up, down)):
            at = pl.ds(0 if s == 0 else rows - 2, 2)
            total = row_terms(halo[:, :, whole], row_band.at[s], xrow)
            middle[n, s] = image[at, inner, whole] + total[:, inner]
            flank[n, at, 0:EDGE] = flank[n, at, 0:EDGE] + total[:, 0:EDGE]
            flank[n, at, EDGE:] = flank[n, at, EDGE:] + total[:, cols - EDGE :]
            send(middle.at[n, s], at, inner, whole)
        send(flank.at[n, :, 0:EDGE], slice(None), pl.ds(0, EDGE), whole)
        send(flank.at[n, :, EDGE:], slice(None), pl.ds(cols - EDGE, EDGE), whole)
    for copy in copies:
        copy.wait()


def per_device(coefficients, vectors):
    rows, cols, lanes = vectors.shape
    ny = lax.axis_size("gy")
    nx = lax.axis_size("gx")
    group = 128 // cols
    lines = rows // group
    tall = -(-(lines + 1) // 8) * 8
    width = lanes // PARTS
    edge_cells = lines * group * 2 * EDGE
    real = jnp.float32
    half = jnp.bfloat16
    hbm = pl.BlockSpec(memory_space=pltpu.HBM)
    vmem = pl.BlockSpec(memory_space=pltpu.VMEM)
    work = (pltpu.VMEM((8 * cols, STEP), half), pltpu.VMEM((rows + 4, 16, STEP), half))
    found = pl.pallas_call(
        functools.partial(main_kernel, ny, nx),
        out_shape=(
            pltpu.VMEM(vectors.shape, real),
            pltpu.VMEM((25, rows, cols), real),
            pltpu.VMEM((2, cols, lanes), real),
            pltpu.VMEM((2, cols, lanes), real),
            pltpu.VMEM((rows + 4, 8, lanes), real),
            pltpu.VMEM((2, 2 * cols, 256), half),
            pltpu.VMEM((edge_cells, 128), half),
        ),
        in_specs=[hbm, hbm],
        out_specs=(vmem,) * 7,
        scratch_shapes=[
            pltpu.VMEM((9, rows, cols), real),
            pltpu.VMEM(vectors.shape, real),
            pltpu.VMEM((rows + 4, cols, lanes), half),
            pltpu.VMEM((rows + 4, cols, lanes), half),
            pltpu.VMEM((9, tall, 128), real),
            pltpu.VMEM((2, tall, 128), real),
            pltpu.VMEM((2, 9, 1, cols), real),
            pltpu.VMEM((2, tall, 128), real),
            pltpu.VMEM((4, 9, 1, cols), real),
            pltpu.VMEM((4, 1, 128), real),
            pltpu.VMEM((25, tall, 128), real),
            pltpu.VMEM((group, 5, 2, tall, 128), real),
            pltpu.VMEM((lines, group * cols, 256), half),
            pltpu.VMEM((lines, group * cols, 256), half),
            pltpu.VMEM((edge_cells, 128), real),
            *work,
            pltpu.SemaphoreType.REGULAR((2,)),
            pltpu.SemaphoreType.DMA(()),
            pltpu.SemaphoreType.DMA((lines,)),
            pltpu.SemaphoreType.DMA((2, 4)),
            pltpu.SemaphoreType.DMA((2, 2, 4)),
            pltpu.SemaphoreType.DMA((2, 2, PARTS + 2)),
            pltpu.SemaphoreType.DMA((2, 4, 4)),
        ],
        compiler_params=pltpu.CompilerParams(
            collective_id=0, has_side_effects=True, vmem_limit_bytes=44 * 2**20
        ),
    )(*[pltpu.with_memory_space_constraint(a, pltpu.HBM) for a in (coefficients, vectors)])
    steps = width // STEP
    image, normal = pl.pallas_call(
        write_kernel,
        out_shape=(
            jax.ShapeDtypeStruct(vectors.shape, real),
            jax.ShapeDtypeStruct((25, rows, cols), real),
        ),
        in_specs=[vmem] * 7,
        out_specs=(hbm, hbm),
        scratch_shapes=[
            pltpu.VMEM((steps, 2, 2, cols - 2 * EDGE, STEP), real),
            pltpu.VMEM((steps, rows, 2 * EDGE, STEP), real),
            *work,
            pltpu.SemaphoreType.DMA((2 + lines + 4 * steps,)),
        ],
        compiler_params=pltpu.CompilerParams(vmem_limit_bytes=8 * 2**20),
    )(*[pltpu.with_memory_space_constraint(a, pltpu.VMEM) for a in found])
    return (normal, image)


def solution(mesh):
    in_specs = (P(None, "gy", "gx"), P("gy", "gx", None))
    out_specs = (P(None, "gy", "gx"), P("gy", "gx", None))
    return jax.shard_map(
        per_device, mesh=mesh, in_specs=in_specs, out_specs=out_specs, check_vma=False
    )
```

```python
import functools
import jax
import jax.numpy as jnp
from jax import lax
from jax.experimental import pallas as pl
from jax.experimental.pallas import tpu as pltpu
from jax.sharding import PartitionSpec as P

MESH = pl.DeviceIdType.MESH
PARTS = 2
STEP = 512
EARLY = 640
ROWWAYS = ((1, 0), (-1, 0))
COLWAYS = ((0, 1), (0, -1))
FORWARD = ((1, 0), (0, 1))
CORNERS = ((1, 1), (1, -1), (-1, 1), (-1, -1))
EDGE = 8


def slot_of(e, f):
    return (e + 2) * 5 + (f + 2)


def two(value):
    top = value.astype(jnp.bfloat16).astype(jnp.float32)
    return top, value - top


def dot(a, b):
    return jnp.dot(a, b, preferred_element_type=jnp.float32)


def row_terms(halo, band, xrow):
    depth = halo.shape[0] * halo.shape[1]
    top, rest = two(halo.reshape(depth, halo.shape[2]))
    xrow[0:depth] = top.astype(jnp.bfloat16)
    xrow[depth : 2 * depth] = rest.astype(jnp.bfloat16)
    xrow[2 * depth : 3 * depth] = top.astype(jnp.bfloat16)
    return dot(band[...], xrow[...]).reshape(halo.shape)


def gather_side(side, part, xs):
    def gather(r, carry):
        raw = side[pl.ds(r * 4, 4), :, part]
        near = lax.broadcasted_iota(jnp.int32, raw.shape, 1) < 4
        top, rest = two(jnp.where(near, raw, 0.0))
        both = jnp.concatenate([top[:, 0:4], rest[:, 0:4], top], axis=1)
        xs[pl.ds(r * 4, 4)] = both.astype(jnp.bfloat16)
        return carry

    lax.fori_loop(0, side.shape[0] // 4, gather, 0)


def side_terms(g, group, side_band, xs):
    width = xs.shape[2]
    s = xs[pl.ds(g * group, 2 * group)].reshape(2 * group * 16, width)
    count = group * 2 * EDGE
    total = dot(side_band[g * count : (g + 1) * count, :], s)
    return total.reshape(group, 2 * EDGE, width)


def main_kernel(ny, nx, coef_hbm, x_hbm, *refs):
    (
        image, normal, up, down, side, row_band, side_band,
        coef, xbuf, xh, xl, weights, strips, ring, edges, corners, bends, norm,
        sources, high, low, side_raw, xrow, xs,
        greeting, coef_sem, load_sem, strip_sems, row_sems, col_sems, relay_sems,
    ) = refs
    rows, cols, lanes = x_hbm.shape
    group = 128 // cols
    lines = rows // group
    tall = weights.shape[1]
    tiles = 2
    width = lanes // PARTS
    gy = lax.axis_index("gy")
    gx = lax.axis_index("gx")

    def there(dy, dx):
        y = gy + dy
        x = gx + dx
        return (y >= 0) & (y < ny) & (x >= 0) & (x < nx)

    barrier = pltpu.get_barrier_semaphore()
    count = jnp.int32(0)
    for dy, dx in FORWARD:
        count = count + there(-dy, -dx).astype(jnp.int32)

        @pl.when(there(dy, dx))
        def _():
            pl.semaphore_signal(barrier, inc=1, device_id={"gy": gy + dy, "gx": gx + dx}, device_id_type=MESH)

    coef_load = pltpu.make_async_copy(coef_hbm, coef, coef_sem)
    loads = []
    for g in range(lines):
        at = pl.ds(g * group, group)
        loads.append(pltpu.make_async_copy(x_hbm.at[at], xbuf.at[at], load_sem.at[g]))

    def job(send, arrive, source, target, dy, dx, sems, *slot):
        copy = pltpu.make_async_remote_copy(
            source, target, sems.at[(0, *slot)], sems.at[(1, *slot)],
            device_id={"gy": gy + dy, "gx": gx + dx}, device_id_type=MESH,
        )
        return send, arrive, copy

    def start(jobs):
        for send, _, copy in jobs:

            @pl.when(send)
            def _():
                copy.start()

    def await_greeting(n):
        @pl.when(there(*FORWARD[n]))
        def _():
            pl.semaphore_wait(greeting.at[n], 1)

    def arrived(jobs):
        for _, arrive, copy in jobs:

            @pl.when(arrive)
            def _():
                copy.wait_recv()

    mine = {1: pl.ds(rows - 2, 2), -1: pl.ds(0, 2)}
    held = {1: pl.ds(rows, 2), -1: pl.ds(2, 2)}
    land = {1: pl.ds(0, 2), -1: pl.ds(rows + 2, 2)}
    spot = {1: pl.ds(0, 2), -1: pl.ds(2, 2)}
    last = {1: pl.ds(cols - 2, 2), -1: pl.ds(0, 2)}
    odd = gx % 2
    early = EARLY
    near = pl.ds(pl.multiple_of((1 - odd) * (cols - EDGE), EDGE), EDGE)
    far = pl.ds(pl.multiple_of(odd * EDGE, EDGE), cols - EDGE)
    row_strips, col_strips, row_near, row_far, col_ends, col_bulk = [], [], [], [[], [], []], [], [[], []]
    for n, (dy, dx) in enumerate(ROWWAYS):
        send, arrive = there(dy, dx), there(-dy, -dx)
        halo = up if dy > 0 else down
        row_strips.append(job(
            send, arrive, coef_hbm.at[:, pl.ds(rows - 1 if dy > 0 else 0, 1)], ring.at[n], dy, dx, strip_sems, n
        ))
        row_near.append(job(
            send, arrive, x_hbm.at[mine[dy], near], halo.at[:, near], dy, dx, row_sems, n, 0
        ))
        for m, (begin, size) in enumerate(((0, early), (early, width - early), (width, lanes - width))):
            part = pl.ds(begin, size)
            row_far[m].append(job(
                send, arrive, x_hbm.at[mine[dy], far, part], halo.at[:, far, part], dy, dx, row_sems, n, m + 1
            ))
    for n, (dy, dx) in enumerate(COLWAYS):
        send, arrive = there(dy, dx), there(-dy, -dx)
        col_strips.append(job(send, arrive, strips.at[n], edges.at[n], dy, dx, strip_sems, n + 2))
        for m, way in enumerate((1, -1)):
            col_ends.append(job(
                send, arrive, x_hbm.at[mine[way], last[dx]], side.at[held[way], spot[dx]], dy, dx, col_sems, n, m
            ))
        for m in range(PARTS):
            part = pl.ds(m * width, width)
            col_bulk[m].append(job(
                send, arrive, x_hbm.at[pl.ds(2, rows - 4), last[dx], part],
                side.at[pl.ds(4, rows - 4), spot[dx], part], dy, dx, col_sems, n, m + 2
            ))
    turn_x, turn_y, corner_x, corner_y = [], [], [], []
    for n, (dy, dx) in enumerate(CORNERS):
        carrier = odd == (0 if dx > 0 else 1)
        by_x = carrier & there(-dy, 0) & there(0, dx)
        by_y = carrier & there(0, -dx) & there(dy, 0)
        whole = there(-dy, -dx)
        from_x = whole & jnp.logical_not(carrier)
        from_y = whole & carrier
        halo = up if dy > 0 else down
        target = side.at[land[dy], spot[dx]]
        turn_x.append(job(by_x, from_x, halo.at[:, last[dx]], target, 0, dx, relay_sems, n, 0))
        turn_y.append(job(by_y, from_y, side.at[held[dy], spot[dx]], target, dy, 0, relay_sems, n, 1))
        corner_x.append(job(
            by_x, from_x, ring.at[0 if dy > 0 else 1], corners.at[n], 0, dx, relay_sems, n, 2
        ))
        source = edges.at[0 if dx > 0 else 1, pl.ds(lines if dy > 0 else 0, 1)]
        corner_y.append(job(by_y, from_y, source, bends.at[n], dy, 0, relay_sems, n, 3))

    dense = (tall, 128)
    line = lax.broadcasted_iota(jnp.int32, dense, 0)
    lane = lax.broadcasted_iota(jnp.int32, dense, 1)
    place = lane // cols
    column = lane % cols
    row_pos = gy * rows + group * line - 2 + place

    @pl.when(count > 0)
    def _():
        pl.semaphore_wait(barrier, count)

    for n, (dy, dx) in enumerate(FORWARD):

        @pl.when(there(-dy, -dx))
        def _():
            pl.semaphore_signal(
                greeting.at[n], inc=1, device_id={"gy": gy - dy, "gx": gx - dx}, device_id_type=MESH
            )

    start([row_strips[1], row_near[1], row_far[0][1], *col_ends[2:4]])
    coef_load.start()
    for g in (0, lines - 1):
        loads[g].start()
    coef_load.wait()
    weights[...] = jnp.zeros_like(weights)
    first = [((i - 2) % group, 0 if i >= 2 else 1) for i in range(group)]
    for k in range(9):
        for i, (row, h) in enumerate(first):
            weights[k, pl.ds(h, lines), i * cols : (i + 1) * cols] = coef[k, pl.ds(row, lines, stride=group), :]
    for s in range(2):
        strip = jnp.zeros(dense, jnp.float32)
        for k in range(9):
            moved = pltpu.roll(weights[k], (k - (cols - 1) * (1 - s)) % 128, 1)
            strip = jnp.where(column == k, moved, strip)
        strips[s] = strip

    for load in loads[1 : lines - 1]:
        load.start()
    start([col_strips[1], col_bulk[0][1], col_bulk[1][1]])
    await_greeting(0)
    start([row_strips[0], row_near[0], row_far[0][0]])
    await_greeting(1)
    start([*col_ends[0:2], col_strips[0], col_bulk[0][0], col_bulk[1][0]])
    loads[0].wait()
    loads[lines - 1].wait()

    for target, dy in ((up, 1), (down, -1)):

        @pl.when(jnp.logical_not(there(-dy, 0)))
        def _():
            target[...] = jnp.zeros_like(target)

    for dx in (1, -1):

        @pl.when(jnp.logical_not(there(0, -dx)))
        def _():
            side[2 : rows + 2, spot[dx]] = jnp.zeros((rows, 2, lanes), jnp.float32)

        for dy in (1, -1):

            @pl.when(jnp.logical_not(there(-dy, -dx)))
            def _():
                side[land[dy], spot[dx]] = jnp.zeros((2, 2, lanes), jnp.float32)

    blank = jnp.zeros((2,) + xh.shape[1:], jnp.bfloat16)
    for ref in (xh, xl):
        ref[0:2] = blank
        ref[rows + 2 : rows + 4] = blank

    for g in (0, lines - 1, *range(1, lines // 2)):
        if 0 < g < lines - 1:
            loads[g].wait()

        def split(n, carry):
            part = pl.ds(pl.multiple_of(n * STEP, STEP), STEP)
            top, rest = two(xbuf[g * group : (g + 1) * group, :, part])
            xh[g * group + 2 : (g + 1) * group + 2, :, part] = top.astype(jnp.bfloat16)
            xl[g * group + 2 : (g + 1) * group + 2, :, part] = rest.astype(jnp.bfloat16)
            return carry

        lax.fori_loop(0, lanes // STEP, split, 0)

    arrived(col_strips + col_ends)
    start(corner_y + turn_y + row_far[1] + row_far[2])
    arrived(row_strips)
    start(corner_x)

    for g in range(lines // 2, lines - 1):
        if 0 < g < lines - 1:
            loads[g].wait()

        def split(n, carry):
            part = pl.ds(pl.multiple_of(n * STEP, STEP), STEP)
            top, rest = two(xbuf[g * group : (g + 1) * group, :, part])
            xh[g * group + 2 : (g + 1) * group + 2, :, part] = top.astype(jnp.bfloat16)
            xl[g * group + 2 : (g + 1) * group + 2, :, part] = rest.astype(jnp.bfloat16)
            return carry

        lax.fori_loop(0, lanes // STEP, split, 0)


    def inside(a, b, col_pos):
        row = row_pos + a
        col = col_pos + b
        return (row >= 0) & (row < ny * rows) & (col >= 0) & (col < nx * cols)

    def down_rows(value, a):
        if a == 0:
            return value
        moved = pltpu.roll(value, (a * cols) % 128, 1)
        crossed = pltpu.roll(moved, a % tall, 0)
        return jnp.where(place == (0 if a > 0 else group - 1), crossed, moved)

    def assemble(sides):
        col_pos = gx * cols + column
        kept = []
        for k in range(9):
            a = k // 3 - 1
            b = k % 3 - 1
            own = jnp.where(inside(a, b, col_pos), weights[k], 0.0)
            before = pltpu.roll(sides[0], (-k) % 128, 1)
            before = jnp.where(inside(a, b, gx * cols - 1), before, 0.0)
            after = pltpu.roll(sides[1], (cols - 1 - k) % 128, 1)
            after = jnp.where(inside(a, b, (gx + 1) * cols), after, 0.0)
            right = jnp.where(column == 0, before, pltpu.roll(own, 1, 1))
            left = jnp.where(column == cols - 1, after, pltpu.roll(own, 127, 1))
            kept.append((left, own, right))
        terms = [None] * 25
        for k in range(9):
            a = k // 3 - 1
            b = k % 3 - 1
            moved = [down_rows(kept[m][b + 1], a) for m in range(9)]
            for m in range(9):
                slot = slot_of(m // 3 - k // 3, m % 3 - k % 3)
                product = moved[k] * moved[m]
                terms[slot] = product if terms[slot] is None else terms[slot] + product
        for slot in range(25):
            norm[slot] = terms[slot]

        for rr in range(group):
            for f in range(-2, 3):
                for t in range(tiles):
                    total = jnp.zeros(dense, jnp.float32)
                    for i in range(group):
                        e = t * group + i - 2 - rr
                        if -2 <= e <= 2:
                            total = jnp.where(place == i, norm[slot_of(-e, -f)], total)
                    sources[rr, f + 2, t] = total

    shape = (cols, 128)
    lane_b = lax.broadcasted_iota(jnp.int32, shape, 1)
    offset = lane_b % cols - lax.broadcasted_iota(jnp.int32, shape, 0)

    def band(g, rr, t):
        total = jnp.zeros(shape, jnp.float32)
        for f in range(-2, 3):
            source = sources[rr, f + 2, t, pl.ds(g + t, 1), :]
            total = jnp.where(offset == f, jnp.broadcast_to(source, shape), total)
        return total

    def build(g, carry):
        for rr in range(group):
            for t in range(tiles):
                top, rest = two(band(g, rr, t))
                at = (g, pl.ds(rr * cols, cols), pl.ds(t * 128, 128))
                high[at] = top.astype(jnp.bfloat16)
                low[at] = rest.astype(jnp.bfloat16)
        return carry


    def local(groups):
        def body(n, carry):
            part = pl.ds(pl.multiple_of(n * STEP, STEP), STEP)
            for g in groups:
                span = pl.ds(g * group, 2 * group)
                h = xh[span, :, part].reshape(2 * group * cols, STEP)
                l = xl[span, :, part].reshape(2 * group * cols, STEP)
                total = dot(high[g], h) + dot(low[g], h) + dot(high[g], l)
                image[pl.ds(g * group, group), :, part] = total.reshape(group, cols, STEP)
            return carry

        return body

    sides = [jnp.where(there(0, -dx), edges[n], 0.0) for n, (_, dx) in enumerate(COLWAYS)]
    assemble(sides)
    lax.fori_loop(1, lines - 1, build, 0)
    inner = range(1, lines - 1)
    lax.fori_loop(0, 2, local(inner), 0)
    arrived(row_near)
    start(turn_x)
    lax.fori_loop(2, lanes // STEP, local(inner), 0)
    arrived(corner_y + corner_x)


    ring_place = {1: (0, 1), -1: (lines, 2)}
    for n, (dy, dx) in enumerate(ROWWAYS):
        h, i = ring_place[dy]
        for k in range(9):
            weights[k, pl.ds(h, 1), i * cols : (i + 1) * cols] = jnp.where(there(-dy, -dx), ring[n, k], 0.0)
    for n, (dy, dx) in enumerate(CORNERS):
        h, i = ring_place[dy]
        here = (line == h) & (place == i)
        at = cols - 1 if dx > 0 else 0
        straight = jnp.zeros(dense, jnp.float32)
        for k in range(9):
            value = jnp.broadcast_to(corners[n, k][:, at : at + 1], dense)
            straight = jnp.where(column == k, value, straight)
        carrier = odd == (0 if dx > 0 else 1)
        value = jnp.where(carrier, jnp.broadcast_to(bends[n], dense), straight)
        value = jnp.where(there(-dy, -dx), value, 0.0)
        s = 0 if dx > 0 else 1
        sides[s] = jnp.where(here, value, sides[s])

    assemble(sides)
    for g in (0, lines - 1):
        build(g, 0)
    lax.fori_loop(0, lanes // STEP, local((0, lines - 1)), 0)

    depth = 2 * cols
    for s in range(2):
        for n in range(2):
            value = band(0, n, 0) if s == 0 else band(lines - 1, group - 2 + n, 1)
            if s:
                value = pltpu.roll(value, 128 - depth, 1)
            top, rest = two(jnp.where(lane_b < depth, value, 0.0))
            at = pl.ds(n * cols, cols)
            row_band[s, at, 0:128] = (top + pltpu.roll(top, depth, 1)).astype(jnp.bfloat16)
            row_band[s, at, 128:256] = rest.astype(jnp.bfloat16)

    side_raw[...] = jnp.zeros_like(side_raw)
    thin = (lines, 128)
    lane_s = lax.broadcasted_iota(jnp.int32, thin, 1)
    pairs = ((0, 0, -2), (0, 1, -1), (1, 1, -2), (cols - 2, 2, 2), (cols - 1, 2, 1), (cols - 1, 3, 2))
    for rr in range(group):
        h = (rr + 2) // group
        i = (rr + 2) % group
        for c in (0, 1, cols - 2, cols - 1):
            total = jnp.zeros(thin, jnp.float32)
            for own, j, f in pairs:
                if own != c:
                    continue
                for e in range(-2, 3):
                    wanted = (lane_s // 16 == rr + 2 + e) & (lane_s % 4 == j) & (lane_s % 16 < 12)
                    at = i * cols + c
                    value = norm[slot_of(e, f), pl.ds(h, lines), :][:, at : at + 1]
                    total = jnp.where(wanted, jnp.broadcast_to(value, thin), total)
            spot = rr * 2 * EDGE + (c if c < 2 else c - cols + 2 * EDGE)
            side_raw[pl.ds(spot, lines, stride=2 * EDGE * group), :] = total
    top, rest = two(side_raw[...])
    part = lax.broadcasted_iota(jnp.int32, side_raw.shape, 1) % 16
    side_band[...] = jnp.where(part < 8, top, rest).astype(jnp.bfloat16)

    def spread(slot, carry):
        for i, (row, h) in enumerate(first):
            value = norm[slot, pl.ds(h, lines), :]
            normal[slot, pl.ds(row, lines, stride=group), :] = value[:, i * cols : (i + 1) * cols]
        return carry

    lax.fori_loop(0, 25, spread, 0, unroll=5)
    xrow[3 * depth : 4 * depth] = jnp.zeros((depth, STEP), jnp.bfloat16)

    arrived(turn_x + turn_y)
    for n in range(PARTS - 1):
        arrived(row_far[0] + row_far[1] + col_bulk[n])

        def beside(m, carry):
            part = pl.ds(pl.multiple_of(n * width + m * STEP, STEP), STEP)
            for s, halo in enumerate((up, down)):
                at = pl.ds(0 if s == 0 else rows - 2, 2)
                total = row_terms(halo[:, :, part], row_band.at[s], xrow)
                image[at, :, part] = image[at, :, part] + total
            gather_side(side, part, xs)
            for g in range(lines):
                total = side_terms(g, group, side_band, xs)
                at = pl.ds(g * group, group)
                image[at, 0:EDGE, part] = image[at, 0:EDGE, part] + total[:, 0:EDGE]
                image[at, cols - EDGE : cols, part] = image[at, cols - EDGE : cols, part] + total[:, EDGE:]
            return carry

        lax.fori_loop(0, width // STEP, beside, 0)
    def sent(jobs):
        for send, _, copy in jobs:

            @pl.when(send)
            def _():
                copy.wait_send()

    sent(row_strips + col_strips + row_near + col_ends + turn_x + turn_y + corner_x + corner_y)
    sent(row_far[0] + row_far[1] + col_bulk[0])
    arrived(col_bulk[PARTS - 1] + row_far[2])
    sent(col_bulk[PARTS - 1] + row_far[2])


def write_kernel(image, normal, up, down, side, row_band, side_band, image_hbm, normal_hbm, *scratch):
    middle, flank, xrow, xs, sem = scratch
    rows, cols, lanes = image.shape
    group = 128 // cols
    lines = rows // group
    width = lanes // PARTS
    head = lanes - width
    depth = 2 * cols
    inner = slice(EDGE, cols - EDGE)
    copies = []

    def send(source, *at):
        copies.append(pltpu.make_async_copy(source, image_hbm.at[at], sem.at[len(copies)]))
        copies[-1].start()

    copies.append(pltpu.make_async_copy(normal, normal_hbm, sem.at[0]))
    copies[0].start()
    for g in range(lines):
        at = pl.ds(g * group, group)
        send(image.at[at, :, 0:head], at, slice(None), pl.ds(0, head))
    at = pl.ds(2, rows - 4)
    send(image.at[at, inner, head:lanes], at, inner, pl.ds(head, width))

    xrow[3 * depth : 4 * depth] = jnp.zeros((depth, STEP), jnp.bfloat16)
    for n in range(width // STEP):
        whole = pl.ds(head + n * STEP, STEP)
        gather_side(side, whole, xs)
        for g in range(lines):
            at = pl.ds(g * group, group)
            total = side_terms(g, group, side_band, xs)
            flank[n, at, 0:EDGE] = image[at, 0:EDGE, whole] + total[:, 0:EDGE]
            flank[n, at, EDGE:] = image[at, cols - EDGE : cols, whole] + total[:, EDGE:]
        for s, halo in enumerate((up, down)):
            at = pl.ds(0 if s == 0 else rows - 2, 2)
            total = row_terms(halo[:, :, whole], row_band.at[s], xrow)
            middle[n, s] = image[at, inner, whole] + total[:, inner]
            flank[n, at, 0:EDGE] = flank[n, at, 0:EDGE] + total[:, 0:EDGE]
            flank[n, at, EDGE:] = flank[n, at, EDGE:] + total[:, cols - EDGE :]
            send(middle.at[n, s], at, inner, whole)
        send(flank.at[n, :, 0:EDGE], slice(None), pl.ds(0, EDGE), whole)
        send(flank.at[n, :, EDGE:], slice(None), pl.ds(cols - EDGE, EDGE), whole)
    for copy in copies:
        copy.wait()


def per_device(coefficients, vectors):
    rows, cols, lanes = vectors.shape
    ny = lax.axis_size("gy")
    nx = lax.axis_size("gx")
    group = 128 // cols
    lines = rows // group
    tall = -(-(lines + 1) // 8) * 8
    width = lanes // PARTS
    edge_cells = lines * group * 2 * EDGE
    real = jnp.float32
    half = jnp.bfloat16
    hbm = pl.BlockSpec(memory_space=pltpu.HBM)
    vmem = pl.BlockSpec(memory_space=pltpu.VMEM)
    work = (pltpu.VMEM((8 * cols, STEP), half), pltpu.VMEM((rows + 4, 16, STEP), half))
    found = pl.pallas_call(
        functools.partial(main_kernel, ny, nx),
        out_shape=(
            pltpu.VMEM(vectors.shape, real),
            pltpu.VMEM((25, rows, cols), real),
            pltpu.VMEM((2, cols, lanes), real),
            pltpu.VMEM((2, cols, lanes), real),
            pltpu.VMEM((rows + 4, 8, lanes), real),
            pltpu.VMEM((2, 2 * cols, 256), half),
            pltpu.VMEM((edge_cells, 128), half),
        ),
        in_specs=[hbm, hbm],
        out_specs=(vmem,) * 7,
        scratch_shapes=[
            pltpu.VMEM((9, rows, cols), real),
            pltpu.VMEM(vectors.shape, real),
            pltpu.VMEM((rows + 4, cols, lanes), half),
            pltpu.VMEM((rows + 4, cols, lanes), half),
            pltpu.VMEM((9, tall, 128), real),
            pltpu.VMEM((2, tall, 128), real),
            pltpu.VMEM((2, 9, 1, cols), real),
            pltpu.VMEM((2, tall, 128), real),
            pltpu.VMEM((4, 9, 1, cols), real),
            pltpu.VMEM((4, 1, 128), real),
            pltpu.VMEM((25, tall, 128), real),
            pltpu.VMEM((group, 5, 2, tall, 128), real),
            pltpu.VMEM((lines, group * cols, 256), half),
            pltpu.VMEM((lines, group * cols, 256), half),
            pltpu.VMEM((edge_cells, 128), real),
            *work,
            pltpu.SemaphoreType.REGULAR((2,)),
            pltpu.SemaphoreType.DMA(()),
            pltpu.SemaphoreType.DMA((lines,)),
            pltpu.SemaphoreType.DMA((2, 4)),
            pltpu.SemaphoreType.DMA((2, 2, 4)),
            pltpu.SemaphoreType.DMA((2, 2, PARTS + 2)),
            pltpu.SemaphoreType.DMA((2, 4, 4)),
        ],
        compiler_params=pltpu.CompilerParams(
            collective_id=0, has_side_effects=True, vmem_limit_bytes=44 * 2**20
        ),
    )(*[pltpu.with_memory_space_constraint(a, pltpu.HBM) for a in (coefficients, vectors)])
    steps = width // STEP
    image, normal = pl.pallas_call(
        write_kernel,
        out_shape=(
            jax.ShapeDtypeStruct(vectors.shape, real),
            jax.ShapeDtypeStruct((25, rows, cols), real),
        ),
        in_specs=[vmem] * 7,
        out_specs=(hbm, hbm),
        scratch_shapes=[
            pltpu.VMEM((steps, 2, 2, cols - 2 * EDGE, STEP), real),
            pltpu.VMEM((steps, rows, 2 * EDGE, STEP), real),
            *work,
            pltpu.SemaphoreType.DMA((2 + lines + 4 * steps,)),
        ],
        compiler_params=pltpu.CompilerParams(vmem_limit_bytes=8 * 2**20),
    )(*[pltpu.with_memory_space_constraint(a, pltpu.VMEM) for a in found])
    return (normal, image)


def solution(mesh):
    in_specs = (P(None, "gy", "gx"), P("gy", "gx", None))
    out_specs = (P(None, "gy", "gx"), P("gy", "gx", None))
    return jax.shard_map(
        per_device, mesh=mesh, in_specs=in_specs, out_specs=out_specs, check_vma=False
    )
```
